256 devices in a mesh: dp: 2 (over y_hi), tm: 32 (over z, y_lo, core), rows: 4 (over x).
Axes of the slice: x: 4, y: 4 (y_hi: 2, y_lo: 2; y = y_hi * 2 + y_lo), z: 8, core: 2. Of those that a mesh axis runs over, the one named last changes fastest.
Arguments:
- clips: bfloat16 [2, 64, 4, 128, 256], P('dp', 'tm', 'rows'), may hold values from -12 to 12
- weight: bfloat16 [3, 3, 3, 256, 256], replicated, may hold values from -0.078125 to 0.078125
- bias: float32 [256], replicated, may hold values from -1 to 1
- head: float32 [256], replicated, may hold values from -4 to 4
Outputs:
- grad_weight: float32 [3, 3, 3, 256, 256], replicated
- grad_bias: float32 [256], replicated
- grad_head: float32 [256], replicated
The draws below stay inside these ranges and needn't reach their ends.
All inputs are finite; a program needn't handle non-finite values.
Results may differ from the reference program's by a relative error of at most 0.0003.
Values may be sent and summed in bfloat16 or wider, within the bound.
A program may use at most 128 MiB of HBM per device.

```python
import jax
import jax.numpy as jnp
from jax import lax

C = 256
WID = 128
NT = 64
NH = 4
CLIPS = 2


def draw_clips(key, part):
    shape = (CLIPS, NT, NH, WID, C)
    frame_scale = 3.0 ** (jnp.arange(NT, dtype=jnp.float32) / max(NT - 1, 1))
    values = jnp.clip(jax.random.normal(key, shape, jnp.float32), -4.0, 4.0)
    return (values * frame_scale[None, :, None, None, None]).astype(jnp.bfloat16)


def centred(key, shape, width, most, kind=jnp.bfloat16):
    return jnp.clip(width * jax.random.normal(key, shape, jnp.float32), -most, most).astype(kind)


def setup_inputs(seed: int = 0) -> dict:
    seeds = jax.random.split(jax.random.key(seed), 5)
    return {
        "clips": draw_clips(jax.random.fold_in(seeds[4], 71), 0),
        "weight": centred(seeds[1], (3, 3, 3, C, C), (27 * C) ** -0.5, 0.078125),
        "bias": jnp.clip(jax.random.uniform(seeds[2], (C,), jnp.float32, -1.0, 1.0), -1.0, 1.0),
        "head": centred(seeds[3], (C,), 1.0, 4.0, jnp.float32),
    }


penalty_weight = 0.01


def conv_offsets(padded, weight, transpose):
    nclip, tpad, rpad, wpad, chans = padded.shape
    frames, rowsn, cols = tpad - 2, rpad - 2, wpad - 2
    total = jnp.zeros((nclip * frames * rowsn * cols, weight.shape[4]), jnp.float32)
    for a in range(3):
        for b in range(3):
            for d in range(3):
                if transpose:
                    piece = padded[:, 2 - a:2 - a + frames, 2 - b:2 - b + rowsn, 2 - d:2 - d + cols]
                    total = total + lax.dot_general(piece.reshape(-1, chans), weight[a, b, d], (((1,), (1,)), ((), ())), preferred_element_type=jnp.float32)
                else:
                    piece = padded[:, a:a + frames, b:b + rowsn, d:d + cols]
                    total = total + jnp.dot(piece.reshape(-1, chans), weight[a, b, d], preferred_element_type=jnp.float32)
    return total.reshape(nclip, frames, rowsn, cols, -1)


def correlate(padded, right):
    nclip, tpad, rpad, wpad, chans = padded.shape
    frames, rowsn, cols = tpad - 2, rpad - 2, wpad - 2
    right_rows = right.reshape(-1, right.shape[-1])
    blocks = []
    for a in range(3):
        for b in range(3):
            for d in range(3):
                piece = padded[:, a:a + frames, b:b + rowsn, d:d + cols].reshape(-1, chans)
                blocks.append(lax.dot_general(piece, right_rows, (((0,), (0,)), ((), ())), preferred_element_type=jnp.float32))
    return jnp.stack(blocks).reshape(3, 3, 3, chans, right.shape[-1])


def pad_all(field):
    return jnp.pad(field, ((0, 0), (1, 1), (1, 1), (1, 1), (0, 0)))


def reference(clips, weight, bias, head):
    clip_pad = pad_all(clips)
    pre = conv_offsets(clip_pad, weight, False) + bias
    sig = jax.nn.sigmoid(pre)
    slope = sig * (1.0 + pre * (1.0 - sig))
    curve = sig * (1.0 - sig) * (2.0 + pre * (1.0 - 2.0 * sig))
    score_grad = (head * slope).astype(jnp.bfloat16)
    input_grad = conv_offsets(pad_all(score_grad), weight, True).astype(jnp.bfloat16)
    grad_pad = pad_all(input_grad)
    back_grad = penalty_weight * conv_offsets(grad_pad, weight, False)
    pre_grad = back_grad * head * curve
    pre_grad_b = pre_grad.astype(jnp.bfloat16)
    grad_weight = penalty_weight * correlate(grad_pad, score_grad) + correlate(clip_pad, pre_grad_b)
    grad_bias = jnp.sum(pre_grad, axis=(0, 1, 2, 3))
    grad_head = jnp.sum(back_grad * slope, axis=(0, 1, 2, 3))
    return grad_weight, grad_bias, grad_head
```

```python
import functools

import jax
import jax.numpy as jnp
from jax import lax
from jax.experimental import pallas as pl
from jax.experimental.pallas import tpu as pltpu
from jax.sharding import PartitionSpec as P

MESH = pl.DeviceIdType.MESH
F32 = jnp.float32
BF16 = jnp.bfloat16
penalty_weight = 0.01
C = 256
NTM = 32
NREMOTE = 112


def kernel(
    clips_ref, w_hbm, bias_ref, head_ref, gw_hbm, small_ref,
    wv, wt, slabs, xraw, xcat, sraw, shl, shr, scat, graw, ghl, ghr, gcat,
    scells, gcells, vals, acc, slope_s, curve_s, sg_s, pgb_s,
    gh, oh, rc, ra, rb, rz, r2a, r2b, r2c, r3z, r3y,
    wsem, osem, send_sems, recv_sems,
):
    dp = lax.axis_index("dp")
    tm = lax.axis_index("tm")
    x = lax.axis_index("rows")
    core = lax.rem(tm, 2)
    y = dp * 2 + lax.rem(tm // 2, 2)
    z = tm // 4
    has_prev = tm > 0
    has_next = tm < NTM - 1
    has_left = x > 0
    has_right = x < 3

    def dev(xx, yy, zz, cc):
        return (yy // 2, zz * 4 + lax.rem(yy, 2) * 2 + cc, xx)

    def xp(s):
        return lax.rem(x + s, 4)

    def yp(s):
        return lax.rem(y + s, 4)

    def zp(s):
        return lax.rem(z + s, 8)

    other = 1 - core
    partner = dev(x, y, z, other)

    counter = [0]
    sends = []

    def remote(src, dst, target):
        n = counter[0]
        counter[0] += 1
        return pltpu.make_async_remote_copy(
            src_ref=src, dst_ref=dst, send_sem=send_sems.at[n], recv_sem=recv_sems.at[n],
            device_id=target, device_id_type=MESH,
        )

    wcopy = pltpu.make_async_copy(w_hbm, wv, wsem)
    wcopy.start()

    barrier = pltpu.get_barrier_semaphore()

    def greet(target):
        pl.semaphore_signal(barrier, inc=1, device_id=target, device_id_type=MESH)

    greet(partner)
    for s in range(1, 4):
        greet(dev(xp(s), y, z, core))
        greet(dev(x, yp(s), z, core))
    for s in range(1, 8):
        greet(dev(x, y, zp(s), core))

    @pl.when(has_prev)
    def _():
        for s in range(4):
            greet((dp, tm - 1, xp(s)))

    @pl.when(has_next)
    def _():
        for s in range(4):
            greet((dp, tm + 1, xp(s)))

    for f in range(2):
        v = clips_ref[f].astype(F32)
        edge = jnp.zeros((8, C), F32)
        v = jnp.concatenate([edge, v, edge], axis=0)
        for c in range(4):
            slabs[c, f] = v[32 * c:32 * c + 48].astype(BF16)
    xraw[1, x] = slabs[x, 0]
    xraw[2, x] = slabs[x, 1]
    zrow = jnp.zeros((4, 32, 768), BF16)
    for cat in (xcat, scat, gcat):
        cat[:, 0] = zrow
        cat[:, 5] = zrow

    @pl.when(jnp.logical_not(has_prev))
    def _():
        xraw[0] = jnp.zeros((4, 48, C), BF16)
        for raw, hl, hr in ((sraw, shl, shr), (graw, ghl, ghr)):
            raw[0] = jnp.zeros((4, 32, C), BF16)
            hl[0] = jnp.zeros((8, C), F32)
            hr[0] = jnp.zeros((8, C), F32)

    @pl.when(jnp.logical_not(has_next))
    def _():
        xraw[3] = jnp.zeros((4, 48, C), BF16)
        for raw, hl, hr in ((sraw, shl, shr), (graw, ghl, ghr)):
            raw[3] = jnp.zeros((4, 32, C), BF16)
            hl[3] = jnp.zeros((8, C), F32)
            hr[3] = jnp.zeros((8, C), F32)

    @pl.when(jnp.logical_not(has_left))
    def _():
        for hl in (shl, ghl):
            hl[...] = jnp.zeros((4, 8, C), F32)

    @pl.when(jnp.logical_not(has_right))
    def _():
        for hr in (shr, ghr):
            hr[...] = jnp.zeros((4, 8, C), F32)

    for cells in (scells, gcells):
        cells[...] = jnp.zeros((2, 2, 8, C), F32)

    pl.semaphore_wait(
        barrier, 14 + 4 * has_prev.astype(jnp.int32) + 4 * has_next.astype(jnp.int32)
    )

    same = [remote(slabs.at[xp(s)], xraw.at[pl.ds(1, 2), x], (dp, tm, xp(s))) for s in range(1, 4)]
    nxt = [remote(slabs.at[xp(s), 1], xraw.at[0, x], (dp, tm + 1, xp(s))) for s in range(4)]
    prv = [remote(slabs.at[xp(s), 0], xraw.at[3, x], (dp, tm - 1, xp(s))) for s in range(4)]

    def exchange(groups):
        for can_send, _, copies in groups:
            @pl.when(can_send)
            def _():
                for copy in copies:
                    copy.start()
        sends.extend((can_send, copies) for can_send, _, copies in groups)

    def arrive(groups):
        for _, can_receive, copies in groups:
            @pl.when(can_receive)
            def _():
                for copy in copies:
                    copy.wait_recv()

    always = tm >= 0
    first = ((always, always, same), (has_next, has_prev, nxt), (has_prev, has_next, prv))
    exchange(first)
    wcopy.wait()
    for k in range(9):
        a, b = k // 3, k % 3
        for d in range(3):
            src = wv[(2 - a) * 3 + 2 - b, (2 - d) * 256:(3 - d) * 256]
            wt[k, d * 256:(d + 1) * 256] = src.T
    arrive(first)

    def first_cat(n, _):
        f, r = n // 4, lax.rem(n, 4)
        v = xraw[f, r].astype(F32)
        for d in range(3):
            xcat[f, r + 1, :, d * C:(d + 1) * C] = v[7 + d:39 + d].astype(BF16)
        return 0

    lax.fori_loop(0, 16, first_cat, 0)

    def conv(cat, weights):
        acc[...] = jnp.zeros((256, C), F32)

        def body(k, _):
            a, b = k // 3, lax.rem(k, 3)
            lhs = cat[pl.ds(a, 2), pl.ds(b, 4)].reshape(256, 768)
            acc[...] += jnp.dot(lhs, weights[k], preferred_element_type=F32)
            return 0

        lax.fori_loop(0, 9, body, 0)
        return acc[...]

    def halo(value, raw, hl, hr, cells):
        raw[1:3] = value.reshape(2, 4, 32, C)
        vals[...] = value.astype(F32).reshape(2, 4, 32, C)
        for f in range(2):
            for r in range(4):
                cells[0, f, r:r + 1] = vals[f, r, 0:1]
                cells[1, f, r:r + 1] = vals[f, r, 31:32]
        first_cells, last_cells = cells.at[0], cells.at[1]
        groups = (
            (has_next, has_prev, [remote(raw.at[2], raw.at[0], (dp, tm + 1, x))]),
            (has_prev, has_next, [remote(raw.at[1], raw.at[3], (dp, tm - 1, x))]),
            (has_right, has_left, [remote(last_cells, hl.at[pl.ds(1, 2)], (dp, tm, x + 1))]),
            (has_left, has_right, [remote(first_cells, hr.at[pl.ds(1, 2)], (dp, tm, x - 1))]),
            (has_next & has_right, has_prev & has_left, [remote(last_cells.at[1], hl.at[0], (dp, tm + 1, x + 1))]),
            (has_next & has_left, has_prev & has_right, [remote(first_cells.at[1], hr.at[0], (dp, tm + 1, x - 1))]),
            (has_prev & has_right, has_next & has_left, [remote(last_cells.at[0], hl.at[3], (dp, tm - 1, x + 1))]),
            (has_prev & has_left, has_next & has_right, [remote(first_cells.at[0], hr.at[3], (dp, tm - 1, x - 1))]),
        )
        exchange(groups)
        return groups

    def make_cat(raw, hl, hr, cat):
        def body(n, _):
            f, r = n // 4, lax.rem(n, 4)
            b = raw[f, r]
            v = b.astype(F32)
            row = lax.broadcasted_iota(jnp.int32, (32, C), 0)
            low = hl[f, pl.ds(r, 1)]
            high = hr[f, pl.ds(r, 1)]
            cat[f, r + 1, :, 0:C] = jnp.where(row == 0, low, pltpu.roll(v, 1, 0)).astype(BF16)
            cat[f, r + 1, :, C:2 * C] = b
            cat[f, r + 1, :, 2 * C:3 * C] = jnp.where(row == 31, high, pltpu.roll(v, 31, 0)).astype(BF16)
            return 0

        lax.fori_loop(0, 16, body, 0)

    pre = conv(xcat, wv) + bias_ref[...]
    sig = jax.nn.sigmoid(pre)
    slope = sig * (1.0 + pre * (1.0 - sig))
    slope_s[...] = slope
    curve_s[...] = sig * (1.0 - sig) * (2.0 + pre * (1.0 - 2.0 * sig))
    sg = (head_ref[...] * slope).astype(BF16)
    sg_s[...] = sg
    groups = halo(sg, sraw, shl, shr, scells)
    arrive(groups)
    make_cat(sraw, shl, shr, scat)
    ig = conv(scat, wt).astype(BF16)
    groups = halo(ig, graw, ghl, ghr, gcells)
    arrive(groups)
    make_cat(graw, ghl, ghr, gcat)
    back = penalty_weight * conv(gcat, wv)
    pre_grad = back * head_ref[...] * curve_s[...]
    pgb_s[...] = pre_grad.astype(BF16)
    bias_row = jnp.sum(pre_grad, axis=0, keepdims=True)
    head_row = jnp.sum(back * slope_s[...], axis=0, keepdims=True)

    def correlate(k, _):
        a, b = k // 3, lax.rem(k, 3)
        dims = (((0,), (0,)), ((), ()))
        g = gcat[pl.ds(a, 2), pl.ds(b, 4)].reshape(256, 768)
        total = penalty_weight * lax.dot_general(g, sg_s[...], dims, preferred_element_type=F32)
        g = xcat[pl.ds(a, 2), pl.ds(b, 4)].reshape(256, 768)
        total += lax.dot_general(g, pgb_s[...], dims, preferred_element_type=F32)
        for d in range(3):
            tap = 3 * k + d
            for h in range(2):
                gh[h, tap // 4, lax.rem(tap, 4)] = total[
                    d * 256:(d + 1) * 256, h * 128:(h + 1) * 128
                ].reshape(4, 8, 8, 128)
        return 0

    spans = ((0, 3), (3, 3), (6, 1))
    zero = []
    for n, (lo, hi) in enumerate(((0, 4), (4, 8), (8, 9))):
        lax.fori_loop(lo, hi, correlate, 0)
        if n == 2:
            tile = lax.broadcasted_iota(jnp.int32, (8, 128), 0)
            for h in range(2):
                gh[h, 6, 3] = jnp.zeros((4, 8, 8, 128), F32)
                gh[h, 6, 3, 0, 0] = jnp.where(
                    tile == 0, bias_row[:, h * 128:(h + 1) * 128],
                    jnp.where(tile == 1, head_row[:, h * 128:(h + 1) * 128], 0.0),
                )
        span = pl.ds(*spans[n])
        copy = remote(gh.at[other, span], rc.at[span], partner)
        copy.start()
        sends.append((always, [copy]))
        zero.append(copy)

    def launch(copies):
        for copy in copies:
            copy.start()
        sends.append((always, copies))

    def landed(copies):
        for copy in copies:
            copy.wait_recv()

    def add_core(n):
        zero[n].wait_recv()

        def body(j, _):
            gh[core, j] += rc[j]
            return 0

        lax.fori_loop(spans[n][0], spans[n][0] + spans[n][1], body, 0)

    mine = gh.at[core]
    A, B = pl.ds(0, 3), pl.ds(3, 3)
    AB = pl.ds(0, 6)
    add_core(0)
    one_a = [remote(mine.at[A, xp(s)], ra.at[s - 1], dev(xp(s), y, z, core)) for s in range(1, 4)]
    launch(one_a)
    add_core(1)
    one_b = [remote(mine.at[B, :, yp(s)], rb.at[s - 1], dev(x, yp(s), z, core)) for s in range(1, 4)]
    launch(one_b)
    add_core(2)
    one_c = [remote(mine.at[6, :, :, zp(s)], rz.at[s - 1], dev(x, y, zp(s), core)) for s in range(1, 8)]
    launch(one_c)

    landed(one_c)
    t = gh[core, 6, :, :, z]
    for s in range(7):
        t += rz[s]
    gh[core, 6, :, :, z] = t
    two_c = [remote(mine.at[6, xp(s), :, z], r2c.at[s - 1], dev(xp(s), y, z, core)) for s in range(1, 4)]
    launch(two_c)
    landed(one_a)
    for j in range(3):
        gh[core, j, x] += ra[0, j] + ra[1, j] + ra[2, j]
    two_a = [remote(mine.at[A, x, yp(s)], r2a.at[s - 1], dev(x, yp(s), z, core)) for s in range(1, 4)]
    launch(two_a)
    landed(one_b)
    for j in range(3):
        gh[core, 3 + j, :, y] += rb[0, j] + rb[1, j] + rb[2, j]
    two_b = [remote(mine.at[B, xp(s), y], r2b.at[s - 1], dev(xp(s), y, z, core)) for s in range(1, 4)]
    launch(two_b)
    landed(two_c)
    gh[core, 6, x, :, z] += r2c[0] + r2c[1] + r2c[2]
    three_c = [remote(mine.at[6, x, yp(s), z], r3y.at[s - 1], dev(x, yp(s), z, core)) for s in range(1, 4)]
    launch(three_c)
    landed(two_a)
    gh[core, 0:3, x, y] += r2a[0] + r2a[1] + r2a[2]
    landed(two_b)
    gh[core, 3:6, x, y] += r2b[0] + r2b[1] + r2b[2]
    three_z = [remote(mine.at[AB, x, y, zp(s)], r3z.at[s - 1], dev(x, y, zp(s), core)) for s in range(1, 8)]
    launch(three_z)

    out = oh.at[core]
    landed(three_c)
    oh[core, 6, x, y, z] = gh[core, 6, x, y, z] + r3y[0] + r3y[1] + r3y[2]
    piece = out.at[6, x, y, z]
    g1c = [remote(piece, piece, dev(x, yp(s), z, core)) for s in range(1, 4)]
    launch(g1c)
    landed(three_z)
    t = gh[core, 0:6, x, y, z]
    for s in range(7):
        t += r3z[s]
    oh[core, 0:6, x, y, z] = t
    piece = out.at[AB, x, y, z]
    g1z = [remote(piece, piece, dev(x, y, zp(s), core)) for s in range(1, 8)]
    launch(g1z)
    landed(g1c)
    piece = out.at[6, x, :, z]
    g2c = [remote(piece, piece, dev(xp(s), y, z, core)) for s in range(1, 4)]
    launch(g2c)
    landed(g1z)
    piece_a = out.at[A, x, y]
    g2a = [remote(piece_a, piece_a, dev(x, yp(s), z, core)) for s in range(1, 4)]
    launch(g2a)
    piece_b = out.at[B, x, y]
    g2b = [remote(piece_b, piece_b, dev(xp(s), y, z, core)) for s in range(1, 4)]
    launch(g2b)
    landed(g2c)
    piece_c = out.at[6, :, :, z]
    g3c = [remote(piece_c, piece_c, dev(x, y, zp(s), core)) for s in range(1, 8)]
    launch(g3c)
    landed(g2a)
    piece_a = out.at[A, x]
    g3a = [remote(piece_a, piece_a, dev(xp(s), y, z, core)) for s in range(1, 4)]
    launch(g3a)
    landed(g2b)
    piece_b = out.at[B, :, y]
    g3b = [remote(piece_b, piece_b, dev(x, yp(s), z, core)) for s in range(1, 4)]
    launch(g3b)
    last = []

    def hand(n):
        span = pl.ds(*spans[n])
        copy = remote(out.at[span], out.at[span], partner)
        launch([copy])
        last.append(copy)

    landed(g3c)
    hand(2)
    landed(g3a)
    hand(0)
    landed(g3b)
    hand(1)
    landed(last)
    writes = []
    for h in range(2):
        small_ref[:, h * 128:(h + 1) * 128] = oh[h, 6, 3, 0, 0]
        for n, (lo, taps) in enumerate(((0, 24), (24, 3))):
            src = oh.at[h, pl.ds(0, 6)] if n == 0 else oh.at[h, 6, pl.ds(0, 3)]
            if n == 0:
                dst = gw_hbm.at[pl.ds(0, 6), :, :, :, :, pl.ds(h * 128, 128)]
            else:
                dst = gw_hbm.at[6, pl.ds(0, 3), :, :, :, pl.ds(h * 128, 128)]
            writes.append(pltpu.make_async_copy(src, dst, osem.at[2 * h + n]))
            writes[-1].start()
    for copy in writes:
        copy.wait()
    for can_send, copies in sends:
        @pl.when(can_send)
        def _():
            for copy in copies:
                copy.wait_send()


def per_device(clips, weight, bias, head):
    vm = pltpu.VMEM
    half = (7, 4, 4, 8, 8, 128)
    field = lambda w: vm((4, 4, w, C), BF16)
    cells = vm((4, 8, C), F32)
    cat = vm((4, 6, 32, 768), BF16)
    plane = vm((256, C), F32)
    scratch = [
        vm((9, 768, C), BF16), vm((9, 768, C), BF16), vm((4, 2, 48, C), BF16), field(48), cat,
        field(32), cells, cells, cat, field(32), cells, cells, cat,
        vm((2, 2, 8, C), F32), vm((2, 2, 8, C), F32), vm((2, 4, 32, C), F32), plane, plane, plane,
        vm((256, C), BF16), vm((256, C), BF16),
        vm((2, *half), F32), vm((2, *half), F32), vm(half, F32),
        vm((3, 3, 4, 8, 8, 128), F32), vm((3, 3, 4, 8, 8, 128), F32), vm((7, 4, 4, 8, 128), F32),
        vm((3, 3, 8, 8, 128), F32), vm((3, 3, 8, 8, 128), F32), vm((3, 4, 8, 128), F32),
        vm((7, 6, 8, 128), F32), vm((3, 8, 128), F32),
        pltpu.SemaphoreType.DMA, pltpu.SemaphoreType.DMA((4,)),
        pltpu.SemaphoreType.DMA((NREMOTE,)), pltpu.SemaphoreType.DMA((NREMOTE,)),
    ]
    inside = pl.BlockSpec(memory_space=pltpu.VMEM)
    outside = pl.BlockSpec(memory_space=pl.ANY)
    gw, small = pl.pallas_call(
        kernel,
        out_shape=(
            jax.ShapeDtypeStruct((7, 4, 4, 8, 8, C), F32),
            jax.ShapeDtypeStruct((8, C), F32),
        ),
        in_specs=[inside, outside, inside, inside],
        out_specs=(outside, inside),
        scratch_shapes=scratch,
        compiler_params=pltpu.CompilerParams(
            collective_id=0, has_side_effects=True, vmem_limit_bytes=60 * 1024 * 1024
        ),
        name="section",
    )(clips.reshape(2, 128, C), weight.reshape(9, 768, C), bias.reshape(1, C), head.reshape(1, C))
    grad_weight = gw.reshape(28, C, C)[:27].reshape(3, 3, 3, C, C)
    return grad_weight, small[0], small[1]


def solution(mesh):
    return jax.shard_map(
        per_device,
        mesh=mesh,
        in_specs=(P("dp", "tm", "rows", None, None), P(), P(), P()),
        out_specs=(P(), P(), P()),
        check_vma=False,
    )
```

```python
import functools

import jax
import jax.numpy as jnp
from jax import lax
from jax.experimental import pallas as pl
from jax.experimental.pallas import tpu as pltpu
from jax.sharding import PartitionSpec as P

MESH = pl.DeviceIdType.MESH
F32 = jnp.float32
BF16 = jnp.bfloat16
penalty_weight = 0.01
C = 256
NTM = 32
NREMOTE = 192


POWER = 16.0
SHIFT = 120.0
SPAN = 1200.0


def kernel(
    clips_hbm, w_hbm, bias_hbm, head_hbm, out_ref, small_ref,
    clips_ref, bias_ref, head_ref, wv, wt, slabs, xraw, xcat, sraw, shl, shr, scat, graw, ghl, ghr, gcat,
    scells, gcells, vals, acc, slope_s, curve_s, sg_s, pgb_s,
    xt, gt, xg, gg, ex, eg, rs_s, rs_p, total, gh, code,
    ry1, rz1, ry2, rz2, meta, mg, my, mz,
    local_sems, send_sems, recv_sems,
):
    dp = lax.axis_index("dp")
    tm = lax.axis_index("tm")
    x = lax.axis_index("rows")
    core = lax.rem(tm, 2)
    y = dp * 2 + lax.rem(tm // 2, 2)
    z = tm // 4
    has_prev = tm > 0
    has_next = tm < NTM - 1
    has_left = x > 0
    has_right = x < 3

    def dev(xx, yy, zz, cc):
        return (yy // 2, zz * 4 + lax.rem(yy, 2) * 2 + cc, xx)

    def xp(s):
        return lax.rem(x + s, 4)

    def yp(s):
        return lax.rem(y + s, 4)

    def zp(s):
        return lax.rem(z + s, 8)

    partner = dev(x, y, z, 1 - core)
    group = x * 2 + core
    chip = tm - core
    chip_prev = chip > 0
    chip_next = chip < NTM - 2

    def gp(s):
        return lax.rem(group + s, 8)

    def peer(s):
        return dev(gp(s) // 2, y, z, lax.rem(gp(s), 2))

    counter = [0]
    sends = []

    def remote(src, dst, target, recv=None):
        n = counter[0]
        counter[0] += 1
        assert n < NREMOTE
        return pltpu.make_async_remote_copy(
            src_ref=src, dst_ref=dst, send_sem=send_sems.at[n],
            recv_sem=recv_sems.at[n if recv is None else recv],
            device_id=target, device_id_type=MESH,
        )

    clips_in, bias_in, head_in, wcopy = arguments = [
        pltpu.make_async_copy(src, dst, local_sems.at[n])
        for n, (src, dst) in enumerate(
            ((clips_hbm, clips_ref), (bias_hbm, bias_ref), (head_hbm, head_ref), (w_hbm, wv))
        )
    ]
    for copy in arguments:
        copy.start()

    barrier = pltpu.get_barrier_semaphore()

    def greet(target):
        pl.semaphore_signal(barrier, inc=1, device_id=target, device_id_type=MESH)

    for s in range(1, 8):
        greet(peer(s))
        greet(dev(x, y, zp(s), core))
    for s in range(1, 4):
        greet(dev(x, yp(s), z, core))

    @pl.when(chip_prev)
    def _():
        for s in range(4):
            for q in range(2):
                greet((dp, chip - 2 + q, xp(s)))

    @pl.when(chip_next)
    def _():
        for s in range(4):
            for q in range(2):
                greet((dp, chip + 2 + q, xp(s)))

    zrow = jnp.zeros((4, 32, 768), BF16)
    for cat in (xcat, scat, gcat):
        cat[:, 0] = zrow
        cat[:, 5] = zrow

    @pl.when(jnp.logical_not(has_prev))
    def _():
        xraw[0] = jnp.zeros((4, 48, C), BF16)
        for raw, hl, hr in ((sraw, shl, shr), (graw, ghl, ghr)):
            raw[0] = jnp.zeros((4, 32, C), BF16)
            hl[0] = jnp.zeros((8, C), F32)
            hr[0] = jnp.zeros((8, C), F32)

    @pl.when(jnp.logical_not(has_next))
    def _():
        xraw[3] = jnp.zeros((4, 48, C), BF16)
        for raw, hl, hr in ((sraw, shl, shr), (graw, ghl, ghr)):
            raw[3] = jnp.zeros((4, 32, C), BF16)
            hl[3] = jnp.zeros((8, C), F32)
            hr[3] = jnp.zeros((8, C), F32)

    @pl.when(jnp.logical_not(has_left))
    def _():
        for hl in (shl, ghl):
            hl[...] = jnp.zeros((4, 8, C), F32)

    @pl.when(jnp.logical_not(has_right))
    def _():
        for hr in (shr, ghr):
            hr[...] = jnp.zeros((4, 8, C), F32)

    @pl.when(jnp.logical_not(chip_prev))
    def _():
        for field in (xg, gg):
            field[0] = jnp.zeros((4, 32, 128), BF16)

    @pl.when(jnp.logical_not(chip_next))
    def _():
        for field in (xg, gg):
            field[5] = jnp.zeros((4, 32, 128), BF16)

    for cells in (scells, gcells):
        cells[...] = jnp.zeros((2, 2, 8, C), F32)

    clips_in.wait()
    for f in range(2):
        v = clips_ref[f].astype(F32)
        edge = jnp.zeros((8, C), F32)
        v = jnp.concatenate([edge, v, edge], axis=0)
        for c in range(4):
            slabs[c, f] = v[32 * c:32 * c + 48].astype(BF16)
    xraw[1, x] = slabs[x, 0]
    xraw[2, x] = slabs[x, 1]
    pl.semaphore_wait(
        barrier, 17 + 8 * chip_prev.astype(jnp.int32) + 8 * chip_next.astype(jnp.int32)
    )

    same = [remote(slabs.at[xp(s)], xraw.at[pl.ds(1, 2), x], (dp, tm, xp(s))) for s in range(1, 4)]
    nxt = [remote(slabs.at[xp(s), 1], xraw.at[0, x], (dp, tm + 1, xp(s))) for s in range(4)]
    prv = [remote(slabs.at[xp(s), 0], xraw.at[3, x], (dp, tm - 1, xp(s))) for s in range(4)]

    def exchange(groups):
        for can_send, _, copies in groups:
            @pl.when(can_send)
            def _():
                for copy in copies:
                    copy.start()
        sends.extend((can_send, copies) for can_send, _, copies in groups)

    def arrive(groups):
        for _, can_receive, copies in groups:
            @pl.when(can_receive)
            def _():
                for copy in copies:
                    copy.wait_recv()

    always = tm >= 0
    first = ((always, always, same), (has_next, has_prev, nxt), (has_prev, has_next, prv))
    exchange(first)
    bias_in.wait()
    head_in.wait()
    wcopy.wait()
    for k in range(9):
        a, b = k // 3, k % 3
        for d in range(3):
            src = wv[(2 - a) * 3 + 2 - b, (2 - d) * 256:(3 - d) * 256]
            wt[k, d * 256:(d + 1) * 256] = src.T
    arrive(first)

    def first_cat(n, _):
        f, r = n // 4, lax.rem(n, 4)
        v = xraw[f, r].astype(F32)
        for d in range(3):
            xcat[f, r + 1, :, d * C:(d + 1) * C] = v[7 + d:39 + d].astype(BF16)
        return 0

    lax.fori_loop(0, 16, first_cat, 0)

    def conv(cat, weights):
        acc[...] = jnp.zeros((256, C), F32)

        def body(k, _):
            a, b = k // 3, lax.rem(k, 3)
            lhs = cat[pl.ds(a, 2), pl.ds(b, 4)].reshape(256, 768)
            acc[...] += jnp.dot(lhs, weights[k], preferred_element_type=F32)
            return 0

        lax.fori_loop(0, 9, body, 0)
        return acc[...]

    def halo(value, raw, hl, hr, cells):
        raw[1:3] = value.reshape(2, 4, 32, C)
        vals[...] = value.astype(F32).reshape(2, 4, 32, C)
        for f in range(2):
            for r in range(4):
                cells[0, f, r:r + 1] = vals[f, r, 0:1]
                cells[1, f, r:r + 1] = vals[f, r, 31:32]
        first_cells, last_cells = cells.at[0], cells.at[1]
        groups = (
            (has_next, has_prev, [remote(raw.at[2], raw.at[0], (dp, tm + 1, x))]),
            (has_prev, has_next, [remote(raw.at[1], raw.at[3], (dp, tm - 1, x))]),
            (has_right, has_left, [remote(last_cells, hl.at[pl.ds(1, 2)], (dp, tm, x + 1))]),
            (has_left, has_right, [remote(first_cells, hr.at[pl.ds(1, 2)], (dp, tm, x - 1))]),
            (has_next & has_right, has_prev & has_left, [remote(last_cells.at[1], hl.at[0], (dp, tm + 1, x + 1))]),
            (has_next & has_left, has_prev & has_right, [remote(first_cells.at[1], hr.at[0], (dp, tm + 1, x - 1))]),
            (has_prev & has_right, has_next & has_left, [remote(last_cells.at[0], hl.at[3], (dp, tm - 1, x + 1))]),
            (has_prev & has_left, has_next & has_right, [remote(first_cells.at[0], hr.at[3], (dp, tm - 1, x - 1))]),
        )
        exchange(groups)
        return groups

    def make_cat(raw, hl, hr, cat):
        def body(n, _):
            f, r = n // 4, lax.rem(n, 4)
            b = raw[f, r]
            v = b.astype(F32)
            row = lax.broadcasted_iota(jnp.int32, (32, C), 0)
            low = hl[f, pl.ds(r, 1)]
            high = hr[f, pl.ds(r, 1)]
            cat[f, r + 1, :, 0:C] = jnp.where(row == 0, low, pltpu.roll(v, 1, 0)).astype(BF16)
            cat[f, r + 1, :, C:2 * C] = b
            cat[f, r + 1, :, 2 * C:3 * C] = jnp.where(row == 31, high, pltpu.roll(v, 31, 0)).astype(BF16)
            return 0

        lax.fori_loop(0, 16, body, 0)

    def launch(copies):
        for copy in copies:
            copy.start()
        sends.append((always, copies))

    def landed(copies):
        for copy in copies:
            copy.wait_recv()

    def gather_left(center, turned, field):
        for f in range(2):
            turned[:, f] = center(f).T.reshape(8, 32, 128)
        for f in range(2):
            field[1 + 2 * core + f, x] = turned[group, f]
        near = [
            remote(turned.at[gp(s)], field.at[pl.ds(1 + 2 * core, 2), x], peer(s)) for s in range(1, 8)
        ]
        launch(near)
        up, down = [], []
        for s in range(4):
            for copies, frame, place, base in ((up, 1, 0, chip + 2), (down, 0, 5, chip - 2)):
                recv = None
                for q in range(2):
                    n = counter[0]
                    copies.append(remote(
                        turned.at[xp(s) * 2 + q, frame], field.at[place, x], (dp, base + q, xp(s)), recv
                    ))
                    recv = n if recv is None else recv
        edges = (
            (chip_next & (core == 1), chip_prev, up, up[::2]),
            (chip_prev & (core == 0), chip_next, down, down[::2]),
        )
        exchange(tuple(e[:3] for e in edges))
        return near, tuple((always, e[1], e[3]) for e in edges)

    def gather_right(value, field):
        own = pl.ds(2 * core, 2)
        for f in range(2):
            field[2 * core + f, x] = value[f]
        near = [remote(value, field.at[own, x], dev(xp(s), y, z, core)) for s in range(1, 4)]
        near.append(remote(value, field.at[own, x], partner))
        launch(near)
        hand = [remote(field.at[own, xp(4 - s)], field.at[own, xp(4 - s)], partner) for s in range(1, 4)]
        return near, hand

    def relay(near, hand):
        for copy, onward in zip(near[:3], hand):
            copy.wait_recv()
            onward.start()
        sends.append((always, hand))

    def gathered(near, hand):
        landed(near[3:])
        landed(hand)

    def expand(field, out):
        lane = lax.broadcasted_iota(jnp.int32, (32, 128), 1)
        col = lax.rem(lane, 32)

        def body(fi, _):
            v = [field[fi, c].astype(F32) for c in range(4)]
            none = jnp.zeros((32, 128), F32)
            for c in range(4):
                low = pltpu.roll(v[c - 1], 97, 1) if c > 0 else none
                high = pltpu.roll(v[c + 1], 31, 1) if c < 3 else none
                shifted = (
                    jnp.where(col == 0, low, pltpu.roll(v[c], 1, 1)),
                    v[c],
                    jnp.where(col == 31, high, pltpu.roll(v[c], 127, 1)),
                )
                for d in range(3):
                    w = shifted[d]
                    rows3 = (
                        jnp.where(lane < 32, 0.0, pltpu.roll(w, 32, 1)),
                        w,
                        jnp.where(lane >= 96, 0.0, pltpu.roll(w, 96, 1)),
                    )
                    for b in range(3):
                        out[b * 3 + d, fi, :, c * 128:(c + 1) * 128] = rows3[b].astype(BF16)
            return 0

        lax.fori_loop(0, 6, body, 0)

    def correlate(left, right):
        def body(t, _):
            lhs = left[:, pl.ds(t, 3)].reshape(864, 512)
            total[...] += jnp.dot(lhs, right[t].reshape(512, C), preferred_element_type=F32)
            return 0

        lax.fori_loop(0, 4, body, 0)

    pre = conv(xcat, wv) + bias_ref[...]
    sig = jax.nn.sigmoid(pre)
    slope = sig * (1.0 + pre * (1.0 - sig))
    slope_s[...] = slope
    curve_s[...] = sig * (1.0 - sig) * (2.0 + pre * (1.0 - 2.0 * sig))
    sg = (head_ref[...] * slope).astype(BF16)
    sg_s[...] = sg.reshape(2, 128, C)
    groups = halo(sg, sraw, shl, shr, scells)
    x_near, x_edges = gather_left(lambda f: xcat[1 + f, 1:5, :, C:2 * C].reshape(128, C), xt, xg)
    right_s = gather_right(sg_s, rs_s)
    arrive(groups)
    make_cat(sraw, shl, shr, scat)
    ig = conv(scat, wt).astype(BF16)
    groups = halo(ig, graw, ghl, ghr, gcells)
    relay(*right_s)
    g_near, g_edges = gather_left(lambda f: graw[1 + f].reshape(128, C), gt, gg)
    arrive(groups)
    make_cat(graw, ghl, ghr, gcat)
    back = penalty_weight * conv(gcat, wv)
    pre_grad = back * head_ref[...] * curve_s[...]
    pgb_s[...] = pre_grad.astype(BF16).reshape(2, 128, C)
    right_p = gather_right(pgb_s, rs_p)
    bias_row = jnp.sum(pre_grad, axis=0, keepdims=True)
    head_row = jnp.sum(back * slope_s[...], axis=0, keepdims=True)
    landed(g_near)
    arrive(g_edges)
    expand(gg, eg)
    gathered(*right_s)
    total[...] = jnp.zeros((864, C), F32)
    correlate(eg, rs_s)
    total[...] = penalty_weight * total[...]
    relay(*right_p)
    landed(x_near)
    arrive(x_edges)
    expand(xg, ex)
    gathered(*right_p)
    correlate(ex, rs_p)

    most = jnp.zeros((8, 128), F32)
    for tap in range(27):
        a, b, d = tap // 9, tap // 3 % 3, tap % 3
        n = (b * 3 + d) * 3 + a
        for h in range(2):
            block = total[n * 32:(n + 1) * 32, h * 128:(h + 1) * 128].reshape(4, 8, 128)
            gh[tap // 4, tap % 4, :, h] = block
            most = jnp.maximum(most, jnp.max(jnp.abs(block), axis=0))
    gh[6, 3] = jnp.zeros((4, 2, 8, 128), F32)
    tile = lax.broadcasted_iota(jnp.int32, (8, 128), 0)
    first_tile = jnp.zeros((8, 128), F32) + jnp.max(most)
    for n, row in enumerate((bias_row, head_row)):
        for h in range(2):
            first_tile = jnp.where(tile == 1 + 2 * n + h, row[:, h * 128:(h + 1) * 128], first_tile)

    zi, zh = z // 2, lax.rem(z, 2)
    Z = pl.ds(5, 2)
    y_spans = ((0, 2), (2, 3))
    one_y = [
        [remote(gh.at[pl.ds(*span), yp(s)], ry1.at[s - 1, pl.ds(*span)], dev(x, yp(s), z, core)) for s in range(1, 4)]
        for span in y_spans
    ]
    one_z = [
        remote(gh.at[Z, :, zp(s) // 2, lax.rem(zp(s), 2)], rz1.at[s - 1], dev(x, y, zp(s), core))
        for s in range(1, 8)
    ]
    launch(one_y[0])
    launch(one_z)
    launch(one_y[1])

    def spread(n, slots, me, targets):
        slots[me] = meta[n]
        copies = [remote(meta.at[n], slots.at[me], target) for target in targets]
        launch(copies)
        return copies

    def combine(n, slots, copies):
        landed(copies)
        new = slots[0]
        for s in range(1, slots.shape[0]):
            new = jnp.where(tile == 0, jnp.maximum(new, slots[s]), new + slots[s])
        meta[n + 1] = new

    meta[0] = first_tile
    meta_g = spread(0, mg, group, [peer(s) for s in range(1, 8)])
    combine(0, mg, meta_g)
    meta_y = spread(1, my, y, [dev(x, yp(s), z, core) for s in range(1, 4)])
    landed(one_z)
    t = gh[5:7, :, zi, zh]
    for s in range(7):
        t += rz1[s]
    gh[5:7, :, zi, zh] = t
    two_y = [remote(gh.at[Z, yp(s), zi, zh], ry2.at[s - 1], dev(x, yp(s), z, core)) for s in range(1, 4)]
    launch(two_y)
    combine(1, my, meta_y)
    meta_z = spread(2, mz, z, [dev(x, y, zp(s), core) for s in range(1, 8)])
    two_z = []
    for copies, (start, count) in zip(one_y, y_spans):
        landed(copies)
        for j in range(start, start + count):
            gh[j, y] += ry1[0, j] + ry1[1, j] + ry1[2, j]
        span = pl.ds(start, count)
        two_z.append([
            remote(gh.at[span, y, zp(s) // 2, lax.rem(zp(s), 2)], rz2.at[s - 1, span], dev(x, y, zp(s), core))
            for s in range(1, 8)
        ])
        launch(two_z[-1])
    combine(2, mz, meta_z)
    scale = SPAN / jnp.maximum(jnp.max(jnp.where(tile == 0, meta[3], 0.0)), 1e-30)

    def coded(v):
        u = v * scale
        w = jnp.exp2(POWER * jnp.log2(jnp.abs(u) + 1.0) - SHIFT)
        return jnp.where(u < 0.0, -w, w).astype(BF16)

    landed(two_y)
    t = gh[5:7, y, zi, zh] + ry2[0] + ry2[1] + ry2[2]
    code[5:7, y, x, core, zi, zh] = coded(t)
    piece = code.at[6, y, x, core, zi, zh]
    g1c = [remote(piece, piece, dev(x, yp(s), z, core)) for s in range(1, 4)]
    launch(g1c)
    landed(two_z[0])
    landed(two_z[1])
    t = gh[0:5, y, zi, zh]
    for s in range(7):
        t += rz2[s]
    code[0:5, y, x, core, zi, zh] = coded(t)

    A, B, AB = pl.ds(0, 3), pl.ds(3, 3), pl.ds(0, 6)
    piece = code.at[AB, y, x, core, zi, zh]
    g1z = [remote(piece, piece, dev(x, y, zp(s), core)) for s in range(1, 8)]
    launch(g1z)
    landed(g1c)
    piece = code.at[6, :, x, core, zi, zh]
    g2c = [remote(piece, piece, dev(xp(s), y, z, core)) for s in range(1, 4)]
    launch(g2c)
    landed(g1z)
    piece_a = code.at[A, y, x, core]
    g2a = [remote(piece_a, piece_a, dev(x, yp(s), z, core)) for s in range(1, 4)]
    launch(g2a)
    piece_b = code.at[B, y, x, core]
    g2b = [remote(piece_b, piece_b, dev(xp(s), y, z, core)) for s in range(1, 4)]
    launch(g2b)
    landed(g2c)
    piece_c = code.at[6, :, :, core, zi, zh]
    g3c = [remote(piece_c, piece_c, dev(x, y, zp(s), core)) for s in range(1, 8)]
    launch(g3c)
    landed(g2a)
    piece_a = code.at[A, :, x, core]
    g3a = [remote(piece_a, piece_a, dev(xp(s), y, z, core)) for s in range(1, 4)]
    launch(g3a)
    landed(g2b)
    piece_b = code.at[B, y, :, core]
    g3b = [remote(piece_b, piece_b, dev(x, yp(s), z, core)) for s in range(1, 4)]
    launch(g3b)
    small_ref[...] = jnp.zeros((8, C), F32)
    for h in range(2):
        lanes = slice(h * 128, (h + 1) * 128)
        small_ref[0:1, lanes] = meta[3, 1 + h:2 + h]
        small_ref[1:2, lanes] = meta[3, 3 + h:4 + h]
        small_ref[2:3, lanes] = jnp.zeros((1, 128), F32) + 1.0 / scale
    inverse = 1.0 / scale

    def decode(n, half):
        first, taps = ((0, 12), (12, 12), (24, 3))[n]

        def body(tap, _):
            for xx in range(4):
                for h in range(2):
                    w = code[tap // 4, lax.rem(tap, 4), xx, half, :, h].astype(F32).reshape(32, 128)
                    m = (jnp.exp2((jnp.log2(jnp.abs(w)) + SHIFT) * (1.0 / POWER)) - 1.0) * inverse
                    out_ref[tap, pl.ds(xx * 64 + half * 32, 32), h * 128:(h + 1) * 128] = jnp.where(w < 0.0, -m, m)
            return 0

        lax.fori_loop(first, first + taps, body, 0)

    spans = (A, B, pl.ds(6, 1))
    last = []
    for n, copies in ((2, g3c), (0, g3a), (1, g3b)):
        landed(copies)
        piece = code.at[spans[n], :, :, core]
        last.append((n, remote(piece, piece, partner)))
        launch([last[-1][1]])
    for n, _ in last:
        decode(n, core)
    for n, copy in last:
        copy.wait_recv()
        decode(n, 1 - core)
    for can_send, copies in sends:
        @pl.when(can_send)
        def _():
            for copy in copies:
                copy.wait_send()


PARTS = 9


def put(gw_ref, small_ref, out_hbm, bias_ref, head_ref, sems):
    size = 27 // PARTS
    copies = [
        pltpu.make_async_copy(gw_ref.at[pl.ds(n * size, size)], out_hbm.at[pl.ds(n * size, size)], sems.at[n])
        for n in range(PARTS)
    ]
    for copy in copies:
        copy.start()
    bias_ref[...] = small_ref[0:1]
    head_ref[...] = small_ref[1:2]
    for copy in copies:
        copy.wait()


def per_device(clips, weight, bias, head):
    vm = pltpu.VMEM
    field = lambda w: vm((4, 4, w, C), BF16)
    cells = vm((4, 8, C), F32)
    cat = vm((4, 6, 32, 768), BF16)
    plane = vm((256, C), F32)
    turned, left = vm((8, 2, 32, 128), BF16), vm((6, 4, 32, 128), BF16)
    wide, right = vm((9, 6, 32, 512), BF16), vm((4, 4, 128, C), BF16)
    coded = (7, 4, 4, 2, 4, 2, 8, 128)
    scratch = [
        vm((2, 128, C), BF16), vm((1, C), F32), vm((1, C), F32),
        vm((9, 768, C), BF16), vm((9, 768, C), BF16), vm((4, 2, 48, C), BF16), field(48), cat,
        field(32), cells, cells, cat, field(32), cells, cells, cat,
        vm((2, 2, 8, C), F32), vm((2, 2, 8, C), F32), vm((2, 4, 32, C), F32), plane, plane, plane,
        vm((2, 128, C), BF16), vm((2, 128, C), BF16),
        turned, turned, left, left, wide, wide, right, right, vm((864, C), F32),
        vm((7, 4, 4, 2, 8, 128), F32), vm(coded, BF16),
        vm((3, 5, 4, 2, 8, 128), F32), vm((7, 2, 4, 8, 128), F32), vm((3, 2, 8, 128), F32),
        vm((7, 5, 8, 128), F32),
        vm((4, 8, 128), F32), vm((8, 8, 128), F32), vm((4, 8, 128), F32), vm((8, 8, 128), F32),
        pltpu.SemaphoreType.DMA((4,)),
        pltpu.SemaphoreType.DMA((NREMOTE,)), pltpu.SemaphoreType.DMA((NREMOTE,)),
    ]
    inside = pl.BlockSpec(memory_space=pltpu.VMEM)
    outside = pl.BlockSpec(memory_space=pltpu.HBM)
    gw, small = pl.pallas_call(
        kernel,
        out_shape=(pltpu.VMEM((27, C, C), F32), pltpu.VMEM((8, C), F32)),
        in_specs=[outside] * 4,
        out_specs=(inside, inside),
        scratch_shapes=scratch,
        compiler_params=pltpu.CompilerParams(
            collective_id=0, has_side_effects=True, vmem_limit_bytes=48 * 1024 * 1024
        ),
        name="section",
    )(clips.reshape(2, 128, C), weight.reshape(9, 768, C), bias.reshape(1, C), head.reshape(1, C))
    gw, grad_bias, grad_head = pl.pallas_call(
        put,
        out_shape=(
            jax.ShapeDtypeStruct((27, C, C), F32),
            jax.ShapeDtypeStruct((1, C), F32),
            jax.ShapeDtypeStruct((1, C), F32),
        ),
        in_specs=[inside, inside],
        out_specs=(outside, inside, inside),
        scratch_shapes=[pltpu.SemaphoreType.DMA((PARTS,))],
        compiler_params=pltpu.CompilerParams(vmem_limit_bytes=16 * 1024 * 1024),
        name="put",
    )(gw, small)
    return gw.reshape(3, 3, 3, C, C), grad_bias.reshape(C), grad_head.reshape(C)


def solution(mesh):
    return jax.shard_map(
        per_device,
        mesh=mesh,
        in_specs=(P("dp", "tm", "rows", None, None), P(), P(), P()),
        out_specs=(P(), P(), P()),
        check_vma=False,
    )
```

```python
import functools

import jax
import jax.numpy as jnp
from jax import lax
from jax.experimental import pallas as pl
from jax.experimental.pallas import tpu as pltpu
from jax.sharding import PartitionSpec as P

MESH = pl.DeviceIdType.MESH
F32 = jnp.float32
BF16 = jnp.bfloat16
penalty_weight = 0.01
C = 256
NTM = 32
NREMOTE = 224


POWER = 16.0
SHIFT = 120.0
SPAN = 1200.0


def kernel(
    clips_hbm, w_hbm, bias_hbm, head_hbm, out_ref, small_ref,
    clips_ref, bias_ref, head_ref, wv, wt, slabs, xraw, xcat, sraw, shl, shr, scat, graw, ghl, ghr, gcat,
    scells, gcells, vals, acc, slope_s, curve_s, sg_s, pgb_s,
    xt, gt, xg, gg, ex, eg, rs_s, rs_p, total, gh, code,
    ry1, rz1, ry2, rz2, meta, mg, my, mz,
    local_sems, send_sems, recv_sems,
):
    dp = lax.axis_index("dp")
    tm = lax.axis_index("tm")
    x = lax.axis_index("rows")
    core = lax.rem(tm, 2)
    y = dp * 2 + lax.rem(tm // 2, 2)
    z = tm // 4
    has_prev = tm > 0
    has_next = tm < NTM - 1
    has_left = x > 0
    has_right = x < 3

    def dev(xx, yy, zz, cc):
        return (yy // 2, zz * 4 + lax.rem(yy, 2) * 2 + cc, xx)

    def xp(s):
        return lax.rem(x + s, 4)

    def yp(s):
        return lax.rem(y + s, 4)

    def zp(s):
        return lax.rem(z + s, 8)

    partner = dev(x, y, z, 1 - core)
    group = x * 2 + core
    chip = tm - core
    chip_prev = chip > 0
    chip_next = chip < NTM - 2

    def gp(s):
        return lax.rem(group + s, 8)

    def peer(s):
        return dev(gp(s) // 2, y, z, lax.rem(gp(s), 2))

    counter = [0]
    sends = []

    def remote(src, dst, target, recv=None):
        n = counter[0]
        counter[0] += 1
        assert n < NREMOTE
        return pltpu.make_async_remote_copy(
            src_ref=src, dst_ref=dst, send_sem=send_sems.at[n],
            recv_sem=recv_sems.at[n if recv is None else recv],
            device_id=target, device_id_type=MESH,
        )

    clips_in, bias_in, head_in, wcopy = arguments = [
        pltpu.make_async_copy(src, dst, local_sems.at[n])
        for n, (src, dst) in enumerate(
            ((clips_hbm, clips_ref), (bias_hbm, bias_ref), (head_hbm, head_ref), (w_hbm, wv))
        )
    ]
    for copy in arguments:
        copy.start()

    barrier = pltpu.get_barrier_semaphore()

    def greet(target):
        pl.semaphore_signal(barrier, inc=1, device_id=target, device_id_type=MESH)

    for s in range(1, 8):
        greet(peer(s))
        greet(dev(x, y, zp(s), core))
    for s in range(1, 4):
        greet(dev(x, yp(s), z, core))

    @pl.when(chip_prev)
    def _():
        for s in range(4):
            for q in range(2):
                greet((dp, chip - 2 + q, xp(s)))

    @pl.when(chip_next)
    def _():
        for s in range(4):
            for q in range(2):
                greet((dp, chip + 2 + q, xp(s)))

    zrow = jnp.zeros((4, 32, 768), BF16)
    for cat in (xcat, scat, gcat):
        cat[:, 0] = zrow
        cat[:, 5] = zrow

    @pl.when(jnp.logical_not(has_prev))
    def _():
        xraw[0] = jnp.zeros((4, 48, C), BF16)
        for raw, hl, hr in ((sraw, shl, shr), (graw, ghl, ghr)):
            raw[0] = jnp.zeros((4, 32, C), BF16)
            hl[0] = jnp.zeros((8, C), F32)
            hr[0] = jnp.zeros((8, C), F32)

    @pl.when(jnp.logical_not(has_next))
    def _():
        xraw[3] = jnp.zeros((4, 48, C), BF16)
        for raw, hl, hr in ((sraw, shl, shr), (graw, ghl, ghr)):
            raw[3] = jnp.zeros((4, 32, C), BF16)
            hl[3] = jnp.zeros((8, C), F32)
            hr[3] = jnp.zeros((8, C), F32)

    @pl.when(jnp.logical_not(has_left))
    def _():
        for hl in (shl, ghl):
            hl[...] = jnp.zeros((4, 8, C), F32)

    @pl.when(jnp.logical_not(has_right))
    def _():
        for hr in (shr, ghr):
            hr[...] = jnp.zeros((4, 8, C), F32)

    @pl.when(jnp.logical_not(chip_prev))
    def _():
        for field in (xg, gg):
            field[0] = jnp.zeros((4, 32, 128), BF16)

    @pl.when(jnp.logical_not(chip_next))
    def _():
        for field in (xg, gg):
            field[5] = jnp.zeros((4, 32, 128), BF16)

    for cells in (scells, gcells):
        cells[...] = jnp.zeros((2, 2, 8, C), F32)

    clips_in.wait()
    for f in range(2):
        v = clips_ref[f].astype(F32)
        edge = jnp.zeros((8, C), F32)
        v = jnp.concatenate([edge, v, edge], axis=0)
        for c in range(4):
            slabs[c, f] = v[32 * c:32 * c + 48].astype(BF16)
    xraw[1, x] = slabs[x, 0]
    xraw[2, x] = slabs[x, 1]
    pl.semaphore_wait(
        barrier, 17 + 8 * chip_prev.astype(jnp.int32) + 8 * chip_next.astype(jnp.int32)
    )

    same = [remote(slabs.at[xp(s)], xraw.at[pl.ds(1, 2), x], (dp, tm, xp(s))) for s in range(1, 4)]
    nxt = [remote(slabs.at[xp(s), 1], xraw.at[0, x], (dp, tm + 1, xp(s))) for s in range(4)]
    prv = [remote(slabs.at[xp(s), 0], xraw.at[3, x], (dp, tm - 1, xp(s))) for s in range(4)]

    def exchange(groups):
        for can_send, _, copies in groups:
            @pl.when(can_send)
            def _():
                for copy in copies:
                    copy.start()
        sends.extend((can_send, copies) for can_send, _, copies in groups)

    def arrive(groups):
        for _, can_receive, copies in groups:
            @pl.when(can_receive)
            def _():
                for copy in copies:
                    copy.wait_recv()

    always = tm >= 0
    first = ((always, always, same), (has_next, has_prev, nxt), (has_prev, has_next, prv))
    exchange(first)
    bias_in.wait()
    head_in.wait()
    wcopy.wait()
    for k in range(9):
        a, b = k // 3, k % 3
        for d in range(3):
            src = wv[(2 - a) * 3 + 2 - b, (2 - d) * 256:(3 - d) * 256]
            wt[k, d * 256:(d + 1) * 256] = src.T
    arrive(first)

    def first_cat(n, _):
        f, r = n // 4, lax.rem(n, 4)
        v = xraw[f, r].astype(F32)
        for d in range(3):
            xcat[f, r + 1, :, d * C:(d + 1) * C] = v[7 + d:39 + d].astype(BF16)
        return 0

    lax.fori_loop(0, 16, first_cat, 0)

    def conv(cat, weights):
        acc[...] = jnp.zeros((256, C), F32)

        def body(k, _):
            a, b = k // 3, lax.rem(k, 3)
            lhs = cat[pl.ds(a, 2), pl.ds(b, 4)].reshape(256, 768)
            acc[...] += jnp.dot(lhs, weights[k], preferred_element_type=F32)
            return 0

        lax.fori_loop(0, 9, body, 0)
        return acc[...]

    def halo(value, raw, hl, hr, cells):
        raw[1:3] = value.reshape(2, 4, 32, C)
        vals[...] = value.astype(F32).reshape(2, 4, 32, C)
        for f in range(2):
            for r in range(4):
                cells[0, f, r:r + 1] = vals[f, r, 0:1]
                cells[1, f, r:r + 1] = vals[f, r, 31:32]
        first_cells, last_cells = cells.at[0], cells.at[1]
        groups = (
            (has_next, has_prev, [remote(raw.at[2], raw.at[0], (dp, tm + 1, x))]),
            (has_prev, has_next, [remote(raw.at[1], raw.at[3], (dp, tm - 1, x))]),
            (has_right, has_left, [remote(last_cells, hl.at[pl.ds(1, 2)], (dp, tm, x + 1))]),
            (has_left, has_right, [remote(first_cells, hr.at[pl.ds(1, 2)], (dp, tm, x - 1))]),
            (has_next & has_right, has_prev & has_left, [remote(last_cells.at[1], hl.at[0], (dp, tm + 1, x + 1))]),
            (has_next & has_left, has_prev & has_right, [remote(first_cells.at[1], hr.at[0], (dp, tm + 1, x - 1))]),
            (has_prev & has_right, has_next & has_left, [remote(last_cells.at[0], hl.at[3], (dp, tm - 1, x + 1))]),
            (has_prev & has_left, has_next & has_right, [remote(first_cells.at[0], hr.at[3], (dp, tm - 1, x - 1))]),
        )
        exchange(groups)
        return groups

    def make_cat(raw, hl, hr, cat):
        def body(n, _):
            f, r = n // 4, lax.rem(n, 4)
            b = raw[f, r]
            v = b.astype(F32)
            row = lax.broadcasted_iota(jnp.int32, (32, C), 0)
            low = hl[f, pl.ds(r, 1)]
            high = hr[f, pl.ds(r, 1)]
            cat[f, r + 1, :, 0:C] = jnp.where(row == 0, low, pltpu.roll(v, 1, 0)).astype(BF16)
            cat[f, r + 1, :, C:2 * C] = b
            cat[f, r + 1, :, 2 * C:3 * C] = jnp.where(row == 31, high, pltpu.roll(v, 31, 0)).astype(BF16)
            return 0

        lax.fori_loop(0, 16, body, 0)

    def launch(copies):
        for copy in copies:
            copy.start()
        sends.append((always, copies))

    def landed(copies):
        for copy in copies:
            copy.wait_recv()

    def gather_left(center, turned, field):
        for f in range(2):
            turned[:, f] = center(f).T.reshape(8, 32, 128)
        for f in range(2):
            field[1 + 2 * core + f, x] = turned[group, f]
        near = [
            remote(turned.at[gp(s)], field.at[pl.ds(1 + 2 * core, 2), x], peer(s)) for s in range(1, 8)
        ]
        launch(near)
        up, down = [], []
        for s in range(4):
            for copies, frame, place, base in ((up, 1, 0, chip + 2), (down, 0, 5, chip - 2)):
                recv = None
                for q in range(2):
                    n = counter[0]
                    copies.append(remote(
                        turned.at[xp(s) * 2 + q, frame], field.at[place, x], (dp, base + q, xp(s)), recv
                    ))
                    recv = n if recv is None else recv
        edges = (
            (chip_next & (core == 1), chip_prev, up, up[::2]),
            (chip_prev & (core == 0), chip_next, down, down[::2]),
        )
        exchange(tuple(e[:3] for e in edges))
        return near, tuple((always, e[1], e[3]) for e in edges)

    def gather_right(value, field):
        own = pl.ds(2 * core, 2)
        for f in range(2):
            field[2 * core + f, x] = value[f]
        near = [remote(value, field.at[own, x], dev(xp(s), y, z, core)) for s in range(1, 4)]
        near.append(remote(value, field.at[own, x], partner))
        launch(near)
        hand = [remote(field.at[own, xp(4 - s)], field.at[own, xp(4 - s)], partner) for s in range(1, 4)]
        return near, hand

    def relay(near, hand):
        for copy, onward in zip(near[:3], hand):
            copy.wait_recv()
            onward.start()
        sends.append((always, hand))

    def gathered(near, hand):
        landed(near[3:])
        landed(hand)

    def expand(field, out):
        lane = lax.broadcasted_iota(jnp.int32, (32, 128), 1)
        col = lax.rem(lane, 32)

        def body(fi, _):
            v = [field[fi, c].astype(F32) for c in range(4)]
            none = jnp.zeros((32, 128), F32)
            for c in range(4):
                low = pltpu.roll(v[c - 1], 97, 1) if c > 0 else none
                high = pltpu.roll(v[c + 1], 31, 1) if c < 3 else none
                shifted = (
                    jnp.where(col == 0, low, pltpu.roll(v[c], 1, 1)),
                    v[c],
                    jnp.where(col == 31, high, pltpu.roll(v[c], 127, 1)),
                )
                for d in range(3):
                    w = shifted[d]
                    rows3 = (
                        jnp.where(lane < 32, 0.0, pltpu.roll(w, 32, 1)),
                        w,
                        jnp.where(lane >= 96, 0.0, pltpu.roll(w, 96, 1)),
                    )
                    for b in range(3):
                        out[b * 3 + d, fi, :, c * 128:(c + 1) * 128] = rows3[b].astype(BF16)
            return 0

        lax.fori_loop(0, 6, body, 0)

    def correlate(left, right):
        def body(t, _):
            lhs = left[:, pl.ds(t, 3)].reshape(864, 512)
            total[...] += jnp.dot(lhs, right[t].reshape(512, C), preferred_element_type=F32)
            return 0

        lax.fori_loop(0, 4, body, 0)

    pre = conv(xcat, wv) + bias_ref[...]
    sig = jax.nn.sigmoid(pre)
    slope = sig * (1.0 + pre * (1.0 - sig))
    slope_s[...] = slope
    curve_s[...] = sig * (1.0 - sig) * (2.0 + pre * (1.0 - 2.0 * sig))
    sg = (head_ref[...] * slope).astype(BF16)
    sg_s[...] = sg.reshape(2, 128, C)
    groups = halo(sg, sraw, shl, shr, scells)
    x_near, x_edges = gather_left(lambda f: xcat[1 + f, 1:5, :, C:2 * C].reshape(128, C), xt, xg)
    right_s = gather_right(sg_s, rs_s)
    arrive(groups)
    make_cat(sraw, shl, shr, scat)
    ig = conv(scat, wt).astype(BF16)
    groups = halo(ig, graw, ghl, ghr, gcells)
    g_near, g_edges = gather_left(lambda f: graw[1 + f].reshape(128, C), gt, gg)
    arrive(groups)
    make_cat(graw, ghl, ghr, gcat)
    back = penalty_weight * conv(gcat, wv)
    pre_grad = back * head_ref[...] * curve_s[...]
    pgb_s[...] = pre_grad.astype(BF16).reshape(2, 128, C)
    right_p = gather_right(pgb_s, rs_p)
    relay(*right_s)
    bias_row = jnp.sum(pre_grad, axis=0, keepdims=True)
    head_row = jnp.sum(back * slope_s[...], axis=0, keepdims=True)
    landed(g_near)
    arrive(g_edges)
    expand(gg, eg)
    gathered(*right_s)
    total[...] = jnp.zeros((864, C), F32)
    correlate(eg, rs_s)
    total[...] = penalty_weight * total[...]
    relay(*right_p)
    landed(x_near)
    arrive(x_edges)
    expand(xg, ex)
    gathered(*right_p)
    correlate(ex, rs_p)

    most = jnp.zeros((8, 128), F32)
    for tap in range(27):
        a, b, d = tap // 9, tap // 3 % 3, tap % 3
        n = (b * 3 + d) * 3 + a
        for h in range(2):
            block = total[n * 32:(n + 1) * 32, h * 128:(h + 1) * 128].reshape(4, 8, 128)
            gh[tap // 4, tap % 4, :, h] = block
            most = jnp.maximum(most, jnp.max(jnp.abs(block), axis=0))
    gh[6, 3] = jnp.zeros((4, 2, 8, 128), F32)
    tile = lax.broadcasted_iota(jnp.int32, (8, 128), 0)
    first_tile = jnp.zeros((8, 128), F32) + jnp.max(most)
    for n, row in enumerate((bias_row, head_row)):
        for h in range(2):
            first_tile = jnp.where(tile == 1 + 2 * n + h, row[:, h * 128:(h + 1) * 128], first_tile)

    zi, zh = z // 2, lax.rem(z, 2)
    Z = pl.ds(0, 2)
    y_spans = ((4, 3), (2, 2))
    one_y = [
        [
            remote(gh.at[pl.ds(j, n), yp(s)], ry1.at[s - 1, pl.ds(j - 2, n)], dev(x, yp(s), z, core))
            for s in range(1, 4)
        ]
        for j, n in y_spans
    ]
    one_z = [
        remote(gh.at[Z, :, zp(s) // 2, lax.rem(zp(s), 2)], rz1.at[s - 1], dev(x, y, zp(s), core))
        for s in range(1, 8)
    ]

    def spread(n, slots, me, targets):
        slots[me] = meta[n]
        copies = [remote(meta.at[n], slots.at[me], target) for target in targets]
        launch(copies)
        return copies

    def combine(n, slots, copies):
        landed(copies)
        new = slots[0]
        for s in range(1, slots.shape[0]):
            new = jnp.where(tile == 0, jnp.maximum(new, slots[s]), new + slots[s])
        meta[n + 1] = new

    meta[0] = first_tile
    meta_y = spread(0, my, y, [dev(x, yp(s), z, core) for s in range(1, 4)])
    launch(one_y[0])
    launch(one_z)
    launch(one_y[1])
    combine(0, my, meta_y)
    meta_z = spread(1, mz, z, [dev(x, y, zp(s), core) for s in range(1, 8)])
    two_z = []
    for copies, (start, count) in zip(one_y, y_spans):
        landed(copies)
        for j in range(start, start + count):
            gh[j, y] += ry1[0, j - 2] + ry1[1, j - 2] + ry1[2, j - 2]
        two_z.append([
            remote(
                gh.at[pl.ds(start, count), y, zp(s) // 2, lax.rem(zp(s), 2)],
                rz2.at[s - 1, pl.ds(start - 2, count)], dev(x, y, zp(s), core),
            )
            for s in range(1, 8)
        ])
        launch(two_z[-1])
    landed(one_z)
    t = gh[0:2, :, zi, zh]
    for s in range(7):
        t += rz1[s]
    gh[0:2, :, zi, zh] = t
    two_y = [remote(gh.at[Z, yp(s), zi, zh], ry2.at[s - 1], dev(x, yp(s), z, core)) for s in range(1, 4)]
    launch(two_y)
    combine(1, mz, meta_z)
    meta_g = spread(2, mg, group, [peer(s) for s in range(1, 8)])
    scale = SPAN / jnp.clip(jnp.max(jnp.where(tile == 0, meta[2], 0.0)), 1e-30, 1e30)
    scale = (jnp.zeros((8, 128), F32) + scale).astype(BF16).astype(F32)

    def coded(v):
        u = v * scale
        w = jnp.exp2(POWER * jnp.log2(jnp.abs(u) + 1.0) - SHIFT)
        return jnp.where(u < 0.0, -w, w).astype(BF16)

    def close(n):
        start, count = y_spans[n]
        landed(two_z[n])
        t = gh[start:start + count, y, zi, zh]
        for s in range(7):
            t += rz2[s, start - 2:start - 2 + count]
        return coded(t)

    def pair_z(j):
        piece = code.at[pl.ds(j, 2), y, x, core, zi, zh]
        copies = [remote(piece, piece, dev(x, y, zp(s), core)) for s in range(1, 8)]
        launch(copies)
        return copies

    def pair_two(j):
        a, b = code.at[j, y, x, core], code.at[j + 1, y, x, core]
        copies = [remote(a, a, dev(x, yp(s), z, core)) for s in range(1, 4)]
        copies += [remote(b, b, dev(xp(s), y, z, core)) for s in range(1, 4)]
        launch(copies)
        return copies

    def pair_three(j):
        a, b = code.at[j, :, x, core], code.at[j + 1, y, :, core]
        one = [remote(a, a, dev(xp(s), y, z, core)) for s in range(1, 4)]
        two = [remote(b, b, dev(x, yp(s), z, core)) for s in range(1, 4)]
        launch(one + two)
        return one, two

    t = close(0)
    code[4:6, y, x, core, zi, zh] = t[0:2]
    code[6, y, x, core, zi, zh] = jnp.where(y == 3, scale, t[2].astype(F32)).astype(BF16)
    early = pair_z(5)
    piece = code.at[4, y, x, core, zi, zh]
    c1 = [remote(piece, piece, dev(x, yp(s), z, core)) for s in range(1, 4)]
    launch(c1)
    landed(two_y)
    code[0:2, y, x, core, zi, zh] = coded(gh[0:2, y, zi, zh] + ry2[0] + ry2[1] + ry2[2])
    other = pair_z(0)
    landed(c1)
    piece = code.at[4, :, x, core, zi, zh]
    c2 = [remote(piece, piece, dev(xp(s), y, z, core)) for s in range(1, 4)]
    launch(c2)
    code[2:4, y, x, core, zi, zh] = close(1)
    late = pair_z(2)
    landed(early)
    early = pair_two(5)
    landed(c2)
    piece = code.at[4, :, :, core, zi, zh]
    c3 = [remote(piece, piece, dev(x, y, zp(s), core)) for s in range(1, 8)]
    launch(c3)
    landed(other)
    other = pair_two(0)
    landed(early)
    early = pair_three(5)
    landed(late)
    late = pair_two(2)
    landed(other)
    other = pair_three(0)
    landed(late)
    late_a, late_b = pair_three(2)
    combine(2, mg, meta_g)
    small_ref[...] = jnp.zeros((8, C), F32)
    for h in range(2):
        lanes = slice(h * 128, (h + 1) * 128)
        small_ref[0:1, lanes] = meta[3, 1 + h:2 + h]
        small_ref[1:2, lanes] = meta[3, 3 + h:4 + h]

    def decode(first, js, t0, ts, x0, xs, half):
        def body(n, _):
            j, t, xx = first + n // (ts * xs), t0 + lax.rem(n // xs, ts), x0 + lax.rem(n, xs)
            inverse = 1.0 / code[6, 3, xx, half, 0, 0].astype(F32)[0:1]
            for h in range(2):
                w = code[j, t, xx, half, :, h].astype(F32).reshape(32, 128)
                m = (jnp.exp2((jnp.log2(jnp.abs(w)) + SHIFT) * (1.0 / POWER)) - 1.0) * inverse
                out_ref[j * 4 + t, pl.ds(xx * 64 + half * 32, 32), h * 128:(h + 1) * 128] = jnp.where(w < 0.0, -m, m)
            return 0

        lax.fori_loop(0, js * ts * xs, body, 0)

    handed = []

    def hand(j, js, t, ts, xx, xs):
        piece = code.at[pl.ds(j, js), pl.ds(t, ts), pl.ds(xx, xs), core]
        copy = remote(piece, piece, partner)
        launch([copy])
        handed.append((copy, j, js, t, ts, xx, xs))

    def show(j, js, t, ts, xx, xs, half):
        if j + js == 7:
            decode(5, 1, t, ts, xx, xs, half)
            decode(6, 1, 0, 3, xx, xs, half)
        else:
            decode(j, js, t, ts, xx, xs, half)

    def finish():
        copy, *place = handed.pop(0)
        copy.wait_recv()
        show(*place, 1 - core)

    hand(2, 1, 0, 4, x, 1)
    hand(3, 1, y, 1, 0, 4)
    landed(early[0] + early[1])
    handed, waiting = [], handed
    hand(5, 2, 0, 4, 0, 4)
    show(5, 2, 0, 4, 0, 4, core)
    landed(c3)
    hand(4, 1, 0, 4, 0, 4)
    show(4, 1, 0, 4, 0, 4, core)
    landed(other[0] + other[1])
    hand(0, 2, 0, 4, 0, 4)
    finish()
    handed += waiting
    show(2, 1, 0, 4, x, 1, core)
    show(3, 1, y, 1, 0, 4, core)
    for s in (1, 3, 2):
        late_a[s - 1].wait_recv()
        hand(2, 1, 0, 4, xp(4 - s), 1)
        late_b[s - 1].wait_recv()
        hand(3, 1, yp(4 - s), 1, 0, 4)
        if s == 1:
            show(0, 2, 0, 4, 0, 4, core)
            finish()
        show(2, 1, 0, 4, xp(4 - s), 1, core)
        show(3, 1, yp(4 - s), 1, 0, 4, core)
        if s == 3:
            finish()
    while handed:
        finish()
    for can_send, copies in sends:
        @pl.when(can_send)
        def _():
            for copy in copies:
                copy.wait_send()


PARTS = 9


def put(gw_ref, small_ref, out_hbm, bias_ref, head_ref, sems):
    size = 27 // PARTS
    copies = [
        pltpu.make_async_copy(gw_ref.at[pl.ds(n * size, size)], out_hbm.at[pl.ds(n * size, size)], sems.at[n])
        for n in range(PARTS)
    ]
    for copy in copies:
        copy.start()
    bias_ref[...] = small_ref[0:1]
    head_ref[...] = small_ref[1:2]
    for copy in copies:
        copy.wait()


def per_device(clips, weight, bias, head):
    vm = pltpu.VMEM
    field = lambda w: vm((4, 4, w, C), BF16)
    cells = vm((4, 8, C), F32)
    cat = vm((4, 6, 32, 768), BF16)
    plane = vm((256, C), F32)
    turned, left = vm((8, 2, 32, 128), BF16), vm((6, 4, 32, 128), BF16)
    wide, right = vm((9, 6, 32, 512), BF16), vm((4, 4, 128, C), BF16)
    coded = (7, 4, 4, 2, 4, 2, 8, 128)
    scratch = [
        vm((2, 128, C), BF16), vm((1, C), F32), vm((1, C), F32),
        vm((9, 768, C), BF16), vm((9, 768, C), BF16), vm((4, 2, 48, C), BF16), field(48), cat,
        field(32), cells, cells, cat, field(32), cells, cells, cat,
        vm((2, 2, 8, C), F32), vm((2, 2, 8, C), F32), vm((2, 4, 32, C), F32), plane, plane, plane,
        vm((2, 128, C), BF16), vm((2, 128, C), BF16),
        turned, turned, left, left, wide, wide, right, right, vm((864, C), F32),
        vm((7, 4, 4, 2, 8, 128), F32), vm(coded, BF16),
        vm((3, 5, 4, 2, 8, 128), F32), vm((7, 2, 4, 8, 128), F32), vm((3, 2, 8, 128), F32),
        vm((7, 5, 8, 128), F32),
        vm((4, 8, 128), F32), vm((8, 8, 128), F32), vm((4, 8, 128), F32), vm((8, 8, 128), F32),
        pltpu.SemaphoreType.DMA((4,)),
        pltpu.SemaphoreType.DMA((NREMOTE,)), pltpu.SemaphoreType.DMA((NREMOTE,)),
    ]
    inside = pl.BlockSpec(memory_space=pltpu.VMEM)
    outside = pl.BlockSpec(memory_space=pltpu.HBM)
    gw, small = pl.pallas_call(
        kernel,
        out_shape=(pltpu.VMEM((27, C, C), F32), pltpu.VMEM((8, C), F32)),
        in_specs=[outside] * 4,
        out_specs=(inside, inside),
        scratch_shapes=scratch,
        compiler_params=pltpu.CompilerParams(
            collective_id=0, has_side_effects=True, vmem_limit_bytes=48 * 1024 * 1024
        ),
        name="section",
    )(clips.reshape(2, 128, C), weight.reshape(9, 768, C), bias.reshape(1, C), head.reshape(1, C))
    gw, grad_bias, grad_head = pl.pallas_call(
        put,
        out_shape=(
            jax.ShapeDtypeStruct((27, C, C), F32),
            jax.ShapeDtypeStruct((1, C), F32),
            jax.ShapeDtypeStruct((1, C), F32),
        ),
        in_specs=[inside, inside],
        out_specs=(outside, inside, inside),
        scratch_shapes=[pltpu.SemaphoreType.DMA((PARTS,))],
        compiler_params=pltpu.CompilerParams(vmem_limit_bytes=16 * 1024 * 1024),
        name="put",
    )(gw, small)
    return gw.reshape(3, 3, 3, C, C), grad_bias.reshape(C), grad_head.reshape(C)


def solution(mesh):
    return jax.shard_map(
        per_device,
        mesh=mesh,
        in_specs=(P("dp", "tm", "rows", None, None), P(), P(), P()),
        out_specs=(P(), P(), P()),
        check_vma=False,
    )
```

```python
import functools

import jax
import jax.numpy as jnp
from jax import lax
from jax.experimental import pallas as pl
from jax.experimental.pallas import tpu as pltpu
from jax.sharding import PartitionSpec as P

MESH = pl.DeviceIdType.MESH
F32 = jnp.float32
BF16 = jnp.bfloat16
penalty_weight = 0.01
C = 256
NTM = 32
NREMOTE = 224


POWER = 16.0
SHIFT = 120.0
ROOT = 2.0 ** (SHIFT / POWER)
SPAN = 1200.0


def kernel(
    clips_hbm, w_hbm, bias_hbm, head_hbm, out_ref, bias_out, head_out,
    clips_ref, bias_ref, head_ref, wv, wt, slabs, xraw, xcat, sraw, shl, shr, scat, graw, ghl, ghr, gcat,
    scells, gcells, vals, acc, slope_s, curve_s, sg_s, pgb_s,
    xt, gt, xg, gg, ex, eg, rs_s, rs_p, total, gh, code,
    ry1, rz1, ry2, rz2, meta, mg, my, mz,
    local_sems, send_sems, recv_sems,
):
    dp = lax.axis_index("dp")
    tm = lax.axis_index("tm")
    x = lax.axis_index("rows")
    core = lax.rem(tm, 2)
    y = dp * 2 + lax.rem(tm // 2, 2)
    z = tm // 4
    has_prev = tm > 0
    has_next = tm < NTM - 1
    has_left = x > 0
    has_right = x < 3

    def dev(xx, yy, zz, cc):
        return (yy // 2, zz * 4 + lax.rem(yy, 2) * 2 + cc, xx)

    def xp(s):
        return lax.rem(x + s, 4)

    def yp(s):
        return lax.rem(y + s, 4)

    def zp(s):
        return lax.rem(z + s, 8)

    partner = dev(x, y, z, 1 - core)
    group = x * 2 + core
    chip = tm - core
    chip_prev = chip > 0
    chip_next = chip < NTM - 2

    def gp(s):
        return lax.rem(group + s, 8)

    def peer(s):
        return dev(gp(s) // 2, y, z, lax.rem(gp(s), 2))

    counter = [0]
    sends = []

    def remote(src, dst, target, recv=None):
        n = counter[0]
        counter[0] += 1
        assert n < NREMOTE
        return pltpu.make_async_remote_copy(
            src_ref=src, dst_ref=dst, send_sem=send_sems.at[n],
            recv_sem=recv_sems.at[n if recv is None else recv],
            device_id=target, device_id_type=MESH,
        )

    clips_in, bias_in, head_in, wcopy = arguments = [
        pltpu.make_async_copy(src, dst, local_sems.at[n])
        for n, (src, dst) in enumerate(
            ((clips_hbm, clips_ref), (bias_hbm, bias_ref), (head_hbm, head_ref), (w_hbm, wv))
        )
    ]
    for copy in arguments:
        copy.start()

    barrier = pltpu.get_barrier_semaphore()

    def greet(target):
        pl.semaphore_signal(barrier, inc=1, device_id=target, device_id_type=MESH)

    for s in range(1, 8):
        greet(peer(s))
        greet(dev(x, y, zp(s), core))
    for s in range(1, 4):
        greet(dev(x, yp(s), z, core))

    @pl.when(chip_prev)
    def _():
        for s in range(4):
            for q in range(2):
                greet((dp, chip - 2 + q, xp(s)))

    @pl.when(chip_next)
    def _():
        for s in range(4):
            for q in range(2):
                greet((dp, chip + 2 + q, xp(s)))

    zrow = jnp.zeros((4, 32, 768), BF16)
    for cat in (xcat, scat, gcat):
        cat[:, 0] = zrow
        cat[:, 5] = zrow

    @pl.when(jnp.logical_not(has_prev))
    def _():
        xraw[0] = jnp.zeros((4, 40, C), BF16)
        for raw, hl, hr in ((sraw, shl, shr), (graw, ghl, ghr)):
            raw[0] = jnp.zeros((4, 32, C), BF16)
            hl[0] = jnp.zeros((8, C), F32)
            hr[0] = jnp.zeros((8, C), F32)

    @pl.when(jnp.logical_not(has_next))
    def _():
        xraw[3] = jnp.zeros((4, 40, C), BF16)
        for raw, hl, hr in ((sraw, shl, shr), (graw, ghl, ghr)):
            raw[3] = jnp.zeros((4, 32, C), BF16)
            hl[3] = jnp.zeros((8, C), F32)
            hr[3] = jnp.zeros((8, C), F32)

    @pl.when(jnp.logical_not(has_left))
    def _():
        for hl in (shl, ghl):
            hl[...] = jnp.zeros((4, 8, C), F32)

    @pl.when(jnp.logical_not(has_right))
    def _():
        for hr in (shr, ghr):
            hr[...] = jnp.zeros((4, 8, C), F32)

    @pl.when(jnp.logical_not(chip_prev))
    def _():
        for field in (xg, gg):
            field[0] = jnp.zeros((4, 32, 128), BF16)

    @pl.when(jnp.logical_not(chip_next))
    def _():
        for field in (xg, gg):
            field[5] = jnp.zeros((4, 32, 128), BF16)

    for cells in (scells, gcells):
        cells[...] = jnp.zeros((2, 2, 8, C), F32)

    clips_in.wait()
    for f in range(2):
        v = clips_ref[f].astype(F32)
        edge = jnp.zeros((8, C), F32)
        v = jnp.concatenate([edge, v, edge], axis=0)
        for c in range(4):
            slabs[c, f] = v[32 * c + 7:32 * c + 47].astype(BF16)
    xraw[1, x] = slabs[x, 0]
    xraw[2, x] = slabs[x, 1]
    pl.semaphore_wait(
        barrier, 17 + 8 * chip_prev.astype(jnp.int32) + 8 * chip_next.astype(jnp.int32)
    )

    same = [remote(slabs.at[xp(s)], xraw.at[pl.ds(1, 2), x], (dp, tm, xp(s))) for s in range(1, 4)]
    nxt = [remote(slabs.at[xp(s), 1], xraw.at[0, x], (dp, tm + 1, xp(s))) for s in range(4)]
    prv = [remote(slabs.at[xp(s), 0], xraw.at[3, x], (dp, tm - 1, xp(s))) for s in range(4)]

    def exchange(groups):
        for can_send, _, copies in groups:
            @pl.when(can_send)
            def _():
                for copy in copies:
                    copy.start()
        sends.extend((can_send, copies) for can_send, _, copies in groups)

    def arrive(groups):
        for _, can_receive, copies in groups:
            @pl.when(can_receive)
            def _():
                for copy in copies:
                    copy.wait_recv()

    always = tm >= 0
    first = ((always, always, same), (has_next, has_prev, nxt), (has_prev, has_next, prv))
    exchange(first)
    bias_in.wait()
    head_in.wait()
    wcopy.wait()
    for k in range(9):
        a, b = k // 3, k % 3
        for d in range(3):
            src = wv[(2 - a) * 3 + 2 - b, (2 - d) * 256:(3 - d) * 256]
            wt[k, d * 256:(d + 1) * 256] = src.T
    arrive(first)

    def first_cat(n, _):
        f, r = n // 4, lax.rem(n, 4)
        v = xraw[f, r].astype(F32)
        for d in range(3):
            xcat[f, r + 1, :, d * C:(d + 1) * C] = v[d:32 + d].astype(BF16)
        return 0

    lax.fori_loop(0, 16, first_cat, 0, unroll=4)

    def conv(cat, weights):
        value = None
        for k in range(9):
            a, b = k // 3, k % 3
            lhs = cat[a:a + 2, b:b + 4].reshape(256, 768)
            part = jnp.dot(lhs, weights[k], preferred_element_type=F32)
            value = part if value is None else value + part
        return value

    def halo(value, raw, hl, hr, cells):
        raw[1:3] = value.reshape(2, 4, 32, C)
        vals[...] = value.astype(F32).reshape(2, 4, 32, C)
        for f in range(2):
            for r in range(4):
                cells[0, f, r:r + 1] = vals[f, r, 0:1]
                cells[1, f, r:r + 1] = vals[f, r, 31:32]
        first_cells, last_cells = cells.at[0], cells.at[1]
        groups = (
            (has_next, has_prev, [remote(raw.at[2], raw.at[0], (dp, tm + 1, x))]),
            (has_prev, has_next, [remote(raw.at[1], raw.at[3], (dp, tm - 1, x))]),
            (has_right, has_left, [remote(last_cells, hl.at[pl.ds(1, 2)], (dp, tm, x + 1))]),
            (has_left, has_right, [remote(first_cells, hr.at[pl.ds(1, 2)], (dp, tm, x - 1))]),
            (has_next & has_right, has_prev & has_left, [remote(last_cells.at[1], hl.at[0], (dp, tm + 1, x + 1))]),
            (has_next & has_left, has_prev & has_right, [remote(first_cells.at[1], hr.at[0], (dp, tm + 1, x - 1))]),
            (has_prev & has_right, has_next & has_left, [remote(last_cells.at[0], hl.at[3], (dp, tm - 1, x + 1))]),
            (has_prev & has_left, has_next & has_right, [remote(first_cells.at[0], hr.at[3], (dp, tm - 1, x - 1))]),
        )
        exchange(groups)
        return groups

    def make_cat(raw, hl, hr, cat):
        def body(n, _):
            f, r = n // 4, lax.rem(n, 4)
            b = raw[f, r]
            v = b.astype(F32)
            row = lax.broadcasted_iota(jnp.int32, (32, C), 0)
            low = hl[f, pl.ds(r, 1)]
            high = hr[f, pl.ds(r, 1)]
            cat[f, r + 1, :, 0:C] = jnp.where(row == 0, low, pltpu.roll(v, 1, 0)).astype(BF16)
            cat[f, r + 1, :, C:2 * C] = b
            cat[f, r + 1, :, 2 * C:3 * C] = jnp.where(row == 31, high, pltpu.roll(v, 31, 0)).astype(BF16)
            return 0

        lax.fori_loop(0, 16, body, 0, unroll=4)

    def launch(copies):
        for copy in copies:
            copy.start()
        sends.append((always, copies))

    def landed(copies):
        for copy in copies:
            copy.wait_recv()

    def gather_left(center, turned, field):
        for f in range(2):
            turned[:, f] = center(f).T.reshape(8, 32, 128)
        for f in range(2):
            field[1 + 2 * core + f, x] = turned[group, f]
        near = [
            remote(turned.at[gp(s)], field.at[pl.ds(1 + 2 * core, 2), x], peer(s)) for s in range(1, 8)
        ]
        launch(near)
        up, down = [], []
        for s in range(4):
            for copies, frame, place, base in ((up, 1, 0, chip + 2), (down, 0, 5, chip - 2)):
                recv = None
                for q in range(2):
                    n = counter[0]
                    copies.append(remote(
                        turned.at[xp(s) * 2 + q, frame], field.at[place, x], (dp, base + q, xp(s)), recv
                    ))
                    recv = n if recv is None else recv
        edges = (
            (chip_next & (core == 1), chip_prev, up, up[::2]),
            (chip_prev & (core == 0), chip_next, down, down[::2]),
        )
        exchange(tuple(e[:3] for e in edges))
        return near, tuple((always, e[1], e[3]) for e in edges)

    def gather_right(value, field):
        own = pl.ds(2 * core, 2)
        for f in range(2):
            field[2 * core + f, x] = value[f]
        near = [remote(value, field.at[own, x], dev(xp(s), y, z, core)) for s in range(1, 4)]
        near.append(remote(value, field.at[own, x], partner))
        launch(near)
        hand = [remote(field.at[own, xp(4 - s)], field.at[own, xp(4 - s)], partner) for s in range(1, 4)]
        return near, hand

    def relay(near, hand):
        for copy, onward in zip(near[:3], hand):
            copy.wait_recv()
            onward.start()
        sends.append((always, hand))

    def gathered(near, hand):
        landed(near[3:])
        landed(hand)

    def expand(field, out):
        lane = lax.broadcasted_iota(jnp.int32, (32, 128), 1)
        col = lax.rem(lane, 32)

        def body(fi, _):
            v = [field[fi, c].astype(F32) for c in range(4)]
            none = jnp.zeros((32, 128), F32)
            for c in range(4):
                low = pltpu.roll(v[c - 1], 97, 1) if c > 0 else none
                high = pltpu.roll(v[c + 1], 31, 1) if c < 3 else none
                shifted = (
                    jnp.where(col == 0, low, pltpu.roll(v[c], 1, 1)),
                    v[c],
                    jnp.where(col == 31, high, pltpu.roll(v[c], 127, 1)),
                )
                for d in range(3):
                    w = shifted[d]
                    rows3 = (
                        jnp.where(lane < 32, 0.0, pltpu.roll(w, 32, 1)),
                        w,
                        jnp.where(lane >= 96, 0.0, pltpu.roll(w, 96, 1)),
                    )
                    for b in range(3):
                        out[b * 3 + d, fi, :, c * 128:(c + 1) * 128] = rows3[b].astype(BF16)
            return 0

        lax.fori_loop(0, 6, body, 0)

    def correlate(left, right):
        def body(t, _):
            lhs = left[:, pl.ds(t, 3)].reshape(864, 512)
            total[...] += jnp.dot(lhs, right[t].reshape(512, C), preferred_element_type=F32)
            return 0

        lax.fori_loop(0, 4, body, 0)

    pre = conv(xcat, wv) + bias_ref[...]
    sig = jax.nn.sigmoid(pre)
    slope = sig * (1.0 + pre * (1.0 - sig))
    slope_s[...] = slope
    curve_s[...] = sig * (1.0 - sig) * (2.0 + pre * (1.0 - 2.0 * sig))
    sg = (head_ref[...] * slope).astype(BF16)
    sg_s[...] = sg.reshape(2, 128, C)
    groups = halo(sg, sraw, shl, shr, scells)
    x_near, x_edges = gather_left(lambda f: xcat[1 + f, 1:5, :, C:2 * C].reshape(128, C), xt, xg)
    right_s = gather_right(sg_s, rs_s)
    arrive(groups)
    make_cat(sraw, shl, shr, scat)
    ig = conv(scat, wt).astype(BF16)
    groups = halo(ig, graw, ghl, ghr, gcells)
    g_near, g_edges = gather_left(lambda f: graw[1 + f].reshape(128, C), gt, gg)
    arrive(groups)
    make_cat(graw, ghl, ghr, gcat)
    back = penalty_weight * conv(gcat, wv)
    pre_grad = back * head_ref[...] * curve_s[...]
    pgb_s[...] = pre_grad.astype(BF16).reshape(2, 128, C)
    right_p = gather_right(pgb_s, rs_p)
    relay(*right_s)
    bias_row = jnp.sum(pre_grad, axis=0, keepdims=True)
    head_row = jnp.sum(back * slope_s[...], axis=0, keepdims=True)
    landed(g_near)
    arrive(g_edges)
    expand(gg, eg)
    gathered(*right_s)
    total[...] = jnp.zeros((864, C), F32)
    correlate(eg, rs_s)
    total[...] = penalty_weight * total[...]
    relay(*right_p)
    landed(x_near)
    arrive(x_edges)
    expand(xg, ex)
    gathered(*right_p)
    correlate(ex, rs_p)

    most = jnp.zeros((8, 128), F32)
    for tap in range(27):
        a, b, d = tap // 9, tap // 3 % 3, tap % 3
        n = (b * 3 + d) * 3 + a
        for h in range(2):
            block = total[n * 32:(n + 1) * 32, h * 128:(h + 1) * 128].reshape(4, 8, 128)
            gh[tap // 4, tap % 4, :, h] = block
            most = jnp.maximum(most, jnp.max(jnp.abs(block), axis=0))
    gh[6, 3] = jnp.zeros((4, 2, 8, 128), F32)
    tile = lax.broadcasted_iota(jnp.int32, (8, 128), 0)
    first_tile = jnp.zeros((8, 128), F32) + jnp.max(most)
    for n, row in enumerate((bias_row, head_row)):
        for h in range(2):
            first_tile = jnp.where(tile == 1 + 2 * n + h, row[:, h * 128:(h + 1) * 128], first_tile)

    zi, zh = z // 2, lax.rem(z, 2)
    Z = pl.ds(0, 2)
    y_spans = ((4, 3), (2, 2))
    one_y = [
        [
            remote(gh.at[pl.ds(j, n), yp(s)], ry1.at[s - 1, pl.ds(j - 2, n)], dev(x, yp(s), z, core))
            for s in range(1, 4)
        ]
        for j, n in y_spans
    ]
    one_z = [
        remote(gh.at[Z, :, zp(s) // 2, lax.rem(zp(s), 2)], rz1.at[s - 1], dev(x, y, zp(s), core))
        for s in range(1, 8)
    ]

    def spread(n, slots, me, targets):
        slots[me] = meta[n]
        copies = [remote(meta.at[n], slots.at[me], target) for target in targets]
        launch(copies)
        return copies

    def combine(n, slots, copies):
        landed(copies)
        new = slots[0]
        for s in range(1, slots.shape[0]):
            new = jnp.where(tile == 0, jnp.maximum(new, slots[s]), new + slots[s])
        meta[n + 1] = new

    meta[0] = first_tile
    meta_y = spread(0, my, y, [dev(x, yp(s), z, core) for s in range(1, 4)])
    launch(one_y[0])
    launch(one_z)
    launch(one_y[1])
    combine(0, my, meta_y)
    meta_z = spread(1, mz, z, [dev(x, y, zp(s), core) for s in range(1, 8)])
    two_z = []
    for copies, (start, count) in zip(one_y, y_spans):
        landed(copies)
        for j in range(start, start + count):
            gh[j, y] += ry1[0, j - 2] + ry1[1, j - 2] + ry1[2, j - 2]
        two_z.append([
            remote(
                gh.at[pl.ds(start, count), y, zp(s) // 2, lax.rem(zp(s), 2)],
                rz2.at[s - 1, pl.ds(start - 2, count)], dev(x, y, zp(s), core),
            )
            for s in range(1, 8)
        ])
        launch(two_z[-1])
    landed(one_z)
    t = gh[0:2, :, zi, zh]
    for s in range(7):
        t += rz1[s]
    gh[0:2, :, zi, zh] = t
    two_y = [remote(gh.at[Z, yp(s), zi, zh], ry2.at[s - 1], dev(x, yp(s), z, core)) for s in range(1, 4)]
    launch(two_y)
    combine(1, mz, meta_z)
    meta_g = spread(2, mg, group, [peer(s) for s in range(1, 8)])
    scale = SPAN / jnp.clip(jnp.max(jnp.where(tile == 0, meta[2], 0.0)), 1e-30, 1e30)
    scale = (jnp.zeros((8, 128), F32) + scale).astype(BF16).astype(F32)

    def coded(v):
        u = v * scale
        w = jnp.exp2(POWER * jnp.log2(jnp.abs(u) + 1.0) - SHIFT)
        return jnp.where(u < 0.0, -w, w).astype(BF16)

    def close(n):
        start, count = y_spans[n]
        landed(two_z[n])
        t = gh[start:start + count, y, zi, zh]
        for s in range(7):
            t += rz2[s, start - 2:start - 2 + count]
        return coded(t)

    def pair_z(j):
        piece = code.at[pl.ds(j, 2), y, x, core, zi, zh]
        copies = [remote(piece, piece, dev(x, y, zp(s), core)) for s in range(1, 8)]
        launch(copies)
        return copies

    def pair_two(j):
        a, b = code.at[j, y, x, core], code.at[j + 1, y, x, core]
        copies = [remote(a, a, dev(x, yp(s), z, core)) for s in range(1, 4)]
        copies += [remote(b, b, dev(xp(s), y, z, core)) for s in range(1, 4)]
        launch(copies)
        return copies

    def pair_three(j):
        a, b = code.at[j, :, x, core], code.at[j + 1, y, :, core]
        one = [remote(a, a, dev(xp(s), y, z, core)) for s in range(1, 4)]
        two = [remote(b, b, dev(x, yp(s), z, core)) for s in range(1, 4)]
        launch(one + two)
        return one, two

    t = close(0)
    code[4:6, y, x, core, zi, zh] = t[0:2]
    code[6, y, x, core, zi, zh] = jnp.where(y == 3, scale, t[2].astype(F32)).astype(BF16)
    early = pair_z(5)
    piece = code.at[4, y, x, core, zi, zh]
    c1 = [remote(piece, piece, dev(x, yp(s), z, core)) for s in range(1, 4)]
    launch(c1)
    landed(two_y)
    code[0:2, y, x, core, zi, zh] = coded(gh[0:2, y, zi, zh] + ry2[0] + ry2[1] + ry2[2])
    other = pair_z(0)
    landed(c1)
    piece = code.at[4, :, x, core, zi, zh]
    c2 = [remote(piece, piece, dev(xp(s), y, z, core)) for s in range(1, 4)]
    launch(c2)
    code[2:4, y, x, core, zi, zh] = close(1)
    late = pair_z(2)
    landed(early)
    early = pair_two(5)
    landed(c2)
    piece = code.at[4, :, :, core, zi, zh]
    c3 = [remote(piece, piece, dev(x, y, zp(s), core)) for s in range(1, 8)]
    launch(c3)
    landed(other)
    other = pair_two(0)
    landed(early)
    early = pair_three(5)
    landed(late)
    late = pair_two(2)
    landed(other)
    other = pair_three(0)
    landed(late)
    late_a, late_b = pair_three(2)
    combine(2, mg, meta_g)
    for h in range(2):
        lanes = slice(h * 128, (h + 1) * 128)
        bias_out[:, lanes] = meta[3, 1 + h:2 + h]
        head_out[:, lanes] = meta[3, 3 + h:4 + h]

    def decode(first, js, t0, ts, x0, xs, half):
        def body(n, _):
            j, t, xx = first + n // (ts * xs), t0 + lax.rem(n // xs, ts), x0 + lax.rem(n, xs)
            inverse = 1.0 / code[6, 3, xx, half, 0, 0].astype(F32)[0:1]
            grown = inverse * ROOT
            for h in range(2):
                w = code[j, t, xx, half, :, h].astype(F32).reshape(32, 128)
                m = lax.rsqrt(lax.rsqrt(lax.rsqrt(lax.rsqrt(jnp.abs(w))))) * grown - inverse
                out_ref[j * 4 + t, pl.ds(xx * 64 + half * 32, 32), h * 128:(h + 1) * 128] = jnp.where(w < 0.0, -m, m)
            return 0

        lax.fori_loop(0, js * ts * xs, body, 0, unroll=4 if js * ts * xs % 4 == 0 else 1)

    handed = []

    def hand(j, js, t, ts, xx, xs):
        piece = code.at[pl.ds(j, js), pl.ds(t, ts), pl.ds(xx, xs), core]
        copy = remote(piece, piece, partner)
        launch([copy])
        handed.append((copy, j, js, t, ts, xx, xs))

    def show(j, js, t, ts, xx, xs, half):
        if j + js == 7:
            decode(5, 1, t, ts, xx, xs, half)
            decode(6, 1, 0, 3, xx, xs, half)
        else:
            decode(j, js, t, ts, xx, xs, half)

    def finish():
        copy, *place = handed.pop(0)
        copy.wait_recv()
        show(*place, 1 - core)

    hand(2, 1, 0, 4, x, 1)
    hand(3, 1, y, 1, 0, 4)
    landed(early[0] + early[1])
    handed, waiting = [], handed
    hand(5, 2, 0, 4, 0, 4)
    show(5, 2, 0, 4, 0, 4, core)
    landed(c3)
    hand(4, 1, 0, 4, 0, 4)
    show(4, 1, 0, 4, 0, 4, core)
    landed(other[0] + other[1])
    hand(0, 2, 0, 4, 0, 4)
    finish()
    handed += waiting
    show(2, 1, 0, 4, x, 1, core)
    show(3, 1, y, 1, 0, 4, core)
    for s in (1, 3, 2):
        late_a[s - 1].wait_recv()
        hand(2, 1, 0, 4, xp(4 - s), 1)
        late_b[s - 1].wait_recv()
        hand(3, 1, yp(4 - s), 1, 0, 4)
        if s == 1:
            show(0, 2, 0, 4, 0, 4, core)
            finish()
        show(2, 1, 0, 4, xp(4 - s), 1, core)
        show(3, 1, yp(4 - s), 1, 0, 4, core)
        if s == 3:
            finish()
    while handed:
        finish()
    for can_send, copies in sends:
        @pl.when(can_send)
        def _():
            for copy in copies:
                copy.wait_send()


PARTS = 9


def put(gw_ref, bias_ref, head_ref, out_hbm, bias_hbm, head_hbm, sems):
    size = 27 // PARTS
    copies = [
        pltpu.make_async_copy(gw_ref.at[pl.ds(n * size, size)], out_hbm.at[pl.ds(n * size, size)], sems.at[n])
        for n in range(PARTS)
    ]
    copies.append(pltpu.make_async_copy(bias_ref, bias_hbm, sems.at[PARTS]))
    copies.append(pltpu.make_async_copy(head_ref, head_hbm, sems.at[PARTS + 1]))
    for copy in copies:
        copy.start()
    for copy in copies:
        copy.wait()


def per_device(clips, weight, bias, head):
    vm = pltpu.VMEM
    field = lambda w: vm((4, 4, w, C), BF16)
    cells = vm((4, 8, C), F32)
    cat = vm((4, 6, 32, 768), BF16)
    plane = vm((256, C), F32)
    turned, left = vm((8, 2, 32, 128), BF16), vm((6, 4, 32, 128), BF16)
    wide, right = vm((9, 6, 32, 512), BF16), vm((4, 4, 128, C), BF16)
    coded = (7, 4, 4, 2, 4, 2, 8, 128)
    scratch = [
        vm((2, 128, C), BF16), vm((1, C), F32), vm((1, C), F32),
        vm((9, 768, C), BF16), vm((9, 768, C), BF16), vm((4, 2, 40, C), BF16), field(40), cat,
        field(32), cells, cells, cat, field(32), cells, cells, cat,
        vm((2, 2, 8, C), F32), vm((2, 2, 8, C), F32), vm((2, 4, 32, C), F32), plane, plane, plane,
        vm((2, 128, C), BF16), vm((2, 128, C), BF16),
        turned, turned, left, left, wide, wide, right, right, vm((864, C), F32),
        vm((7, 4, 4, 2, 8, 128), F32), vm(coded, BF16),
        vm((3, 5, 4, 2, 8, 128), F32), vm((7, 2, 4, 8, 128), F32), vm((3, 2, 8, 128), F32),
        vm((7, 5, 8, 128), F32),
        vm((4, 8, 128), F32), vm((8, 8, 128), F32), vm((4, 8, 128), F32), vm((8, 8, 128), F32),
        pltpu.SemaphoreType.DMA((4,)),
        pltpu.SemaphoreType.DMA((NREMOTE,)), pltpu.SemaphoreType.DMA((NREMOTE,)),
    ]
    inside = pl.BlockSpec(memory_space=pltpu.VMEM)
    outside = pl.BlockSpec(memory_space=pltpu.HBM)
    gw, grad_bias, grad_head = pl.pallas_call(
        kernel,
        out_shape=(pltpu.VMEM((27, C, C), F32), pltpu.VMEM((1, C), F32), pltpu.VMEM((1, C), F32)),
        in_specs=[outside] * 4,
        out_specs=(inside, inside, inside),
        scratch_shapes=scratch,
        compiler_params=pltpu.CompilerParams(
            collective_id=0, has_side_effects=True, vmem_limit_bytes=48 * 1024 * 1024
        ),
        name="section",
    )(clips.reshape(2, 128, C), weight.reshape(9, 768, C), bias.reshape(1, C), head.reshape(1, C))
    gw, grad_bias, grad_head = pl.pallas_call(
        put,
        out_shape=(
            jax.ShapeDtypeStruct((27, C, C), F32),
            jax.ShapeDtypeStruct((1, C), F32),
            jax.ShapeDtypeStruct((1, C), F32),
        ),
        in_specs=[inside, inside, inside],
        out_specs=(outside, outside, outside),
        scratch_shapes=[pltpu.SemaphoreType.DMA((PARTS + 2,))],
        compiler_params=pltpu.CompilerParams(vmem_limit_bytes=16 * 1024 * 1024),
        name="put",
    )(gw, grad_bias, grad_head)
    return gw.reshape(3, 3, 3, C, C), grad_bias.reshape(C), grad_head.reshape(C)


def solution(mesh):
    return jax.shard_map(
        per_device,
        mesh=mesh,
        in_specs=(P("dp", "tm", "rows", None, None), P(), P(), P()),
        out_specs=(P(), P(), P()),
        check_vma=False,
    )
```

```python
import functools

import jax
import jax.numpy as jnp
from jax import lax
from jax.experimental import pallas as pl
from jax.experimental.pallas import tpu as pltpu
from jax.sharding import PartitionSpec as P

MESH = pl.DeviceIdType.MESH
F32 = jnp.float32
BF16 = jnp.bfloat16
penalty_weight = 0.01
C = 256
NTM = 32
NREMOTE = 224


POWER = 16.0
SHIFT = 120.0
ROOT = 2.0 ** (SHIFT / POWER)
SPAN = 1200.0


def kernel(
    clips_hbm, w_hbm, bias_hbm, head_hbm, out_ref, bias_out, head_out,
    clips_ref, bias_ref, head_ref, wv, wt, slabs, xraw, xcat, sraw, shl, shr, scat, graw, ghl, ghr, gcat,
    scells, gcells, vals, acc, slope_s, curve_s, sg_s, pgb_s,
    xt, gt, xg, gg, ex, eg, rs_s, rs_p, total, gh, code,
    ry1, rz1, ry2, rz2, meta, mg, my, mz,
    local_sems, send_sems, recv_sems,
):
    dp = lax.axis_index("dp")
    tm = lax.axis_index("tm")
    x = lax.axis_index("rows")
    core = lax.rem(tm, 2)
    y = dp * 2 + lax.rem(tm // 2, 2)
    z = tm // 4
    has_prev = tm > 0
    has_next = tm < NTM - 1
    has_left = x > 0
    has_right = x < 3

    def dev(xx, yy, zz, cc):
        return (yy // 2, zz * 4 + lax.rem(yy, 2) * 2 + cc, xx)

    def xp(s):
        return lax.rem(x + s, 4)

    def yp(s):
        return lax.rem(y + s, 4)

    def zp(s):
        return lax.rem(z + s, 8)

    partner = dev(x, y, z, 1 - core)
    group = x * 2 + core
    chip = tm - core
    chip_prev = chip > 0
    chip_next = chip < NTM - 2

    def gp(s):
        return lax.rem(group + s, 8)

    def peer(s):
        return dev(gp(s) // 2, y, z, lax.rem(gp(s), 2))

    counter = [0]
    sends = []

    def remote(src, dst, target, recv=None):
        n = counter[0]
        counter[0] += 1
        assert n < NREMOTE
        return pltpu.make_async_remote_copy(
            src_ref=src, dst_ref=dst, send_sem=send_sems.at[n],
            recv_sem=recv_sems.at[n if recv is None else recv],
            device_id=target, device_id_type=MESH,
        )

    clips_in, bias_in, head_in, wcopy = arguments = [
        pltpu.make_async_copy(src, dst, local_sems.at[n])
        for n, (src, dst) in enumerate(
            ((clips_hbm, clips_ref), (bias_hbm, bias_ref), (head_hbm, head_ref), (w_hbm, wv))
        )
    ]
    for copy in arguments:
        copy.start()

    barrier = pltpu.get_barrier_semaphore()

    def greet(target):
        pl.semaphore_signal(barrier, inc=1, device_id=target, device_id_type=MESH)

    for s in range(1, 8):
        greet(peer(s))
        greet(dev(x, y, zp(s), core))
    for s in range(1, 4):
        greet(dev(x, yp(s), z, core))

    @pl.when(chip_prev)
    def _():
        for s in range(4):
            for q in range(2):
                greet((dp, chip - 2 + q, xp(s)))

    @pl.when(chip_next)
    def _():
        for s in range(4):
            for q in range(2):
                greet((dp, chip + 2 + q, xp(s)))

    zrow = jnp.zeros((4, 32, 768), BF16)
    for cat in (xcat, scat, gcat):
        cat[:, 0] = zrow
        cat[:, 5] = zrow

    @pl.when(jnp.logical_not(has_prev))
    def _():
        xraw[0] = jnp.zeros((4, 40, C), BF16)
        for raw, hl, hr in ((sraw, shl, shr), (graw, ghl, ghr)):
            raw[0] = jnp.zeros((4, 32, C), BF16)
            hl[0] = jnp.zeros((8, C), F32)
            hr[0] = jnp.zeros((8, C), F32)

    @pl.when(jnp.logical_not(has_next))
    def _():
        xraw[3] = jnp.zeros((4, 40, C), BF16)
        for raw, hl, hr in ((sraw, shl, shr), (graw, ghl, ghr)):
            raw[3] = jnp.zeros((4, 32, C), BF16)
            hl[3] = jnp.zeros((8, C), F32)
            hr[3] = jnp.zeros((8, C), F32)

    @pl.when(jnp.logical_not(has_left))
    def _():
        for hl in (shl, ghl):
            hl[...] = jnp.zeros((4, 8, C), F32)

    @pl.when(jnp.logical_not(has_right))
    def _():
        for hr in (shr, ghr):
            hr[...] = jnp.zeros((4, 8, C), F32)

    @pl.when(jnp.logical_not(chip_prev))
    def _():
        for field in (xg, gg):
            field[0] = jnp.zeros((4, 32, 128), BF16)

    @pl.when(jnp.logical_not(chip_next))
    def _():
        for field in (xg, gg):
            field[5] = jnp.zeros((4, 32, 128), BF16)

    for cells in (scells, gcells):
        cells[...] = jnp.zeros((2, 2, 8, C), F32)

    clips_in.wait()
    for f in range(2):
        v = clips_ref[f].astype(F32)
        edge = jnp.zeros((8, C), F32)
        v = jnp.concatenate([edge, v, edge], axis=0)
        for c in range(4):
            slabs[c, f] = v[32 * c + 7:32 * c + 47].astype(BF16)
    xraw[1, x] = slabs[x, 0]
    xraw[2, x] = slabs[x, 1]
    pl.semaphore_wait(
        barrier, 17 + 8 * chip_prev.astype(jnp.int32) + 8 * chip_next.astype(jnp.int32)
    )

    same = [remote(slabs.at[xp(s)], xraw.at[pl.ds(1, 2), x], (dp, tm, xp(s))) for s in range(1, 4)]
    nxt = [remote(slabs.at[xp(s), 1], xraw.at[0, x], (dp, tm + 1, xp(s))) for s in range(4)]
    prv = [remote(slabs.at[xp(s), 0], xraw.at[3, x], (dp, tm - 1, xp(s))) for s in range(4)]

    def exchange(groups):
        for can_send, _, copies in groups:
            @pl.when(can_send)
            def _():
                for copy in copies:
                    copy.start()
        sends.extend((can_send, copies) for can_send, _, copies in groups)

    def arrive(groups):
        for _, can_receive, copies in groups:
            @pl.when(can_receive)
            def _():
                for copy in copies:
                    copy.wait_recv()

    always = tm >= 0
    first = ((has_next, has_prev, nxt[::-1]), (has_prev, has_next, prv[::-1]), (always, always, same))
    exchange(first)
    bias_in.wait()
    head_in.wait()
    wcopy.wait()
    for k in range(9):
        a, b = k // 3, k % 3
        for d in range(3):
            src = wv[(2 - a) * 3 + 2 - b, (2 - d) * 256:(3 - d) * 256]
            wt[k, d * 256:(d + 1) * 256] = src.T
    arrive(first)

    def first_cat(n, _):
        f, r = n // 4, lax.rem(n, 4)
        v = xraw[f, r].astype(F32)
        for d in range(3):
            xcat[f, r + 1, :, d * C:(d + 1) * C] = v[d:32 + d].astype(BF16)
        return 0

    lax.fori_loop(0, 16, first_cat, 0, unroll=4)

    def conv(cat, weights):
        value = None
        for k in range(9):
            a, b = k // 3, k % 3
            lhs = cat[a:a + 2, b:b + 4].reshape(256, 768)
            part = jnp.dot(lhs, weights[k], preferred_element_type=F32)
            value = part if value is None else value + part
        return value

    def halo(value, raw, hl, hr, cells):
        raw[1:3] = value.reshape(2, 4, 32, C)
        vals[...] = value.astype(F32).reshape(2, 4, 32, C)
        for f in range(2):
            for r in range(4):
                cells[0, f, r:r + 1] = vals[f, r, 0:1]
                cells[1, f, r:r + 1] = vals[f, r, 31:32]
        first_cells, last_cells = cells.at[0], cells.at[1]
        groups = (
            (has_next, has_prev, [remote(raw.at[2], raw.at[0], (dp, tm + 1, x))]),
            (has_prev, has_next, [remote(raw.at[1], raw.at[3], (dp, tm - 1, x))]),
            (has_right, has_left, [remote(last_cells, hl.at[pl.ds(1, 2)], (dp, tm, x + 1))]),
            (has_left, has_right, [remote(first_cells, hr.at[pl.ds(1, 2)], (dp, tm, x - 1))]),
            (has_next & has_right, has_prev & has_left, [remote(last_cells.at[1], hl.at[0], (dp, tm + 1, x + 1))]),
            (has_next & has_left, has_prev & has_right, [remote(first_cells.at[1], hr.at[0], (dp, tm + 1, x - 1))]),
            (has_prev & has_right, has_next & has_left, [remote(last_cells.at[0], hl.at[3], (dp, tm - 1, x + 1))]),
            (has_prev & has_left, has_next & has_right, [remote(first_cells.at[0], hr.at[3], (dp, tm - 1, x - 1))]),
        )
        exchange(groups)
        return groups

    def make_cat(raw, hl, hr, cat):
        def body(n, _):
            f, r = n // 4, lax.rem(n, 4)
            b = raw[f, r]
            v = b.astype(F32)
            row = lax.broadcasted_iota(jnp.int32, (32, C), 0)
            low = hl[f, pl.ds(r, 1)]
            high = hr[f, pl.ds(r, 1)]
            cat[f, r + 1, :, 0:C] = jnp.where(row == 0, low, pltpu.roll(v, 1, 0)).astype(BF16)
            cat[f, r + 1, :, C:2 * C] = b
            cat[f, r + 1, :, 2 * C:3 * C] = jnp.where(row == 31, high, pltpu.roll(v, 31, 0)).astype(BF16)
            return 0

        lax.fori_loop(0, 16, body, 0, unroll=4)

    def launch(copies):
        for copy in copies:
            copy.start()
        sends.append((always, copies))

    def landed(copies):
        for copy in copies:
            copy.wait_recv()

    def gather_left(center, turned, field):
        for f in range(2):
            turned[:, f] = center(f).T.reshape(8, 32, 128)
        for f in range(2):
            field[1 + 2 * core + f, x] = turned[group, f]
        near = [
            remote(turned.at[gp(s)], field.at[pl.ds(1 + 2 * core, 2), x], peer(s)) for s in range(1, 8)
        ]
        launch(near)
        up, down = [], []
        for s in range(4):
            for copies, frame, place, base in ((up, 1, 0, chip + 2), (down, 0, 5, chip - 2)):
                recv = None
                for q in range(2):
                    n = counter[0]
                    copies.append(remote(
                        turned.at[xp(s) * 2 + q, frame], field.at[place, x], (dp, base + q, xp(s)), recv
                    ))
                    recv = n if recv is None else recv
        edges = (
            (chip_next & (core == 1), chip_prev, up, up[::2]),
            (chip_prev & (core == 0), chip_next, down, down[::2]),
        )
        exchange(tuple(e[:3] for e in edges))
        return near, tuple((always, e[1], e[3]) for e in edges)

    def gather_right(value, field):
        own = pl.ds(2 * core, 2)
        for f in range(2):
            field[2 * core + f, x] = value[f]
        near = [remote(value, field.at[own, x], dev(xp(s), y, z, core)) for s in range(1, 4)]
        near.append(remote(value, field.at[own, x], partner))
        launch(near)
        hand = [remote(field.at[own, xp(4 - s)], field.at[own, xp(4 - s)], partner) for s in range(1, 4)]
        return near, hand

    def relay(near, hand):
        for copy, onward in zip(near[:3], hand):
            copy.wait_recv()
            onward.start()
        sends.append((always, hand))

    def gathered(near, hand):
        landed(near[3:])
        landed(hand)

    def expand(field, out):
        lane = lax.broadcasted_iota(jnp.int32, (32, 128), 1)
        col = lax.rem(lane, 32)

        def body(fi, _):
            v = [field[fi, c].astype(F32) for c in range(4)]
            none = jnp.zeros((32, 128), F32)
            for c in range(4):
                low = pltpu.roll(v[c - 1], 97, 1) if c > 0 else none
                high = pltpu.roll(v[c + 1], 31, 1) if c < 3 else none
                shifted = (
                    jnp.where(col == 0, low, pltpu.roll(v[c], 1, 1)),
                    v[c],
                    jnp.where(col == 31, high, pltpu.roll(v[c], 127, 1)),
                )
                for d in range(3):
                    w = shifted[d]
                    rows3 = (
                        jnp.where(lane < 32, 0.0, pltpu.roll(w, 32, 1)),
                        w,
                        jnp.where(lane >= 96, 0.0, pltpu.roll(w, 96, 1)),
                    )
                    for b in range(3):
                        out[b * 3 + d, fi, :, c * 128:(c + 1) * 128] = rows3[b].astype(BF16)
            return 0

        lax.fori_loop(0, 6, body, 0, unroll=2)

    def correlate(left, right):
        def body(t, _):
            lhs = left[:, pl.ds(t, 3)].reshape(864, 512)
            total[...] += jnp.dot(lhs, right[t].reshape(512, C), preferred_element_type=F32)
            return 0

        lax.fori_loop(0, 4, body, 0)

    pre = conv(xcat, wv) + bias_ref[...]
    sig = jax.nn.sigmoid(pre)
    slope = sig * (1.0 + pre * (1.0 - sig))
    slope_s[...] = slope
    curve_s[...] = sig * (1.0 - sig) * (2.0 + pre * (1.0 - 2.0 * sig))
    sg = (head_ref[...] * slope).astype(BF16)
    sg_s[...] = sg.reshape(2, 128, C)
    groups = halo(sg, sraw, shl, shr, scells)
    x_near, x_edges = gather_left(lambda f: xcat[1 + f, 1:5, :, C:2 * C].reshape(128, C), xt, xg)
    right_s = gather_right(sg_s, rs_s)
    arrive(groups)
    make_cat(sraw, shl, shr, scat)
    ig = conv(scat, wt).astype(BF16)
    groups = halo(ig, graw, ghl, ghr, gcells)
    g_near, g_edges = gather_left(lambda f: graw[1 + f].reshape(128, C), gt, gg)
    arrive(groups)
    make_cat(graw, ghl, ghr, gcat)
    back = penalty_weight * conv(gcat, wv)
    pre_grad = back * head_ref[...] * curve_s[...]
    pgb_s[...] = pre_grad.astype(BF16).reshape(2, 128, C)
    right_p = gather_right(pgb_s, rs_p)
    relay(*right_s)
    bias_row = jnp.sum(pre_grad, axis=0, keepdims=True)
    head_row = jnp.sum(back * slope_s[...], axis=0, keepdims=True)
    landed(g_near)
    arrive(g_edges)
    expand(gg, eg)
    gathered(*right_s)
    total[...] = jnp.zeros((864, C), F32)
    correlate(eg, rs_s)
    total[...] = penalty_weight * total[...]
    relay(*right_p)
    landed(x_near)
    arrive(x_edges)
    expand(xg, ex)
    gathered(*right_p)
    correlate(ex, rs_p)

    most = jnp.zeros((8, 128), F32)
    for tap in range(27):
        a, b, d = tap // 9, tap // 3 % 3, tap % 3
        n = (b * 3 + d) * 3 + a
        for h in range(2):
            block = total[n * 32:(n + 1) * 32, h * 128:(h + 1) * 128].reshape(4, 8, 128)
            gh[tap // 4, tap % 4, :, h] = block
            most = jnp.maximum(most, jnp.max(jnp.abs(block), axis=0))
    gh[6, 3] = jnp.zeros((4, 2, 8, 128), F32)
    tile = lax.broadcasted_iota(jnp.int32, (8, 128), 0)
    first_tile = jnp.zeros((8, 128), F32) + jnp.max(most)
    for n, row in enumerate((bias_row, head_row)):
        for h in range(2):
            first_tile = jnp.where(tile == 1 + 2 * n + h, row[:, h * 128:(h + 1) * 128], first_tile)

    zi, zh = z // 2, lax.rem(z, 2)
    Z = pl.ds(0, 2)
    y_spans = ((4, 3), (2, 2))
    one_y = [
        [
            remote(gh.at[pl.ds(j, n), yp(s)], ry1.at[s - 1, pl.ds(j - 2, n)], dev(x, yp(s), z, core))
            for s in range(1, 4)
        ]
        for j, n in y_spans
    ]
    one_z = [
        remote(gh.at[Z, :, zp(s) // 2, lax.rem(zp(s), 2)], rz1.at[s - 1], dev(x, y, zp(s), core))
        for s in range(1, 8)
    ]

    def spread(n, slots, me, targets):
        slots[me] = meta[n]
        copies = [remote(meta.at[n], slots.at[me], target) for target in targets]
        launch(copies)
        return copies

    def combine(n, slots, copies):
        landed(copies)
        new = slots[0]
        for s in range(1, slots.shape[0]):
            new = jnp.where(tile == 0, jnp.maximum(new, slots[s]), new + slots[s])
        meta[n + 1] = new

    meta[0] = first_tile
    meta_y = spread(0, my, y, [dev(x, yp(s), z, core) for s in range(1, 4)])
    launch(one_y[0])
    launch(one_z)
    launch(one_y[1])
    combine(0, my, meta_y)
    meta_z = spread(1, mz, z, [dev(x, y, zp(s), core) for s in range(1, 8)])
    two_z = []
    for copies, (start, count) in zip(one_y, y_spans):
        landed(copies)
        for j in range(start, start + count):
            gh[j, y] += ry1[0, j - 2] + ry1[1, j - 2] + ry1[2, j - 2]
        two_z.append([
            remote(
                gh.at[pl.ds(start, count), y, zp(s) // 2, lax.rem(zp(s), 2)],
                rz2.at[s - 1, pl.ds(start - 2, count)], dev(x, y, zp(s), core),
            )
            for s in range(1, 8)
        ])
        launch(two_z[-1])
    landed(one_z)
    t = gh[0:2, :, zi, zh]
    for s in range(7):
        t += rz1[s]
    gh[0:2, :, zi, zh] = t
    two_y = [remote(gh.at[Z, yp(s), zi, zh], ry2.at[s - 1], dev(x, yp(s), z, core)) for s in range(1, 4)]
    launch(two_y)
    combine(1, mz, meta_z)
    meta_g = spread(2, mg, group, [peer(s) for s in range(1, 8)])
    scale = SPAN / jnp.clip(jnp.max(jnp.where(tile == 0, meta[2], 0.0)), 1e-30, 1e30)
    scale = (jnp.zeros((8, 128), F32) + scale).astype(BF16).astype(F32)

    def coded(v):
        u = v * scale
        w = jnp.exp2(POWER * jnp.log2(jnp.abs(u) + 1.0) - SHIFT)
        return jnp.where(u < 0.0, -w, w).astype(BF16)

    def close(n):
        start, count = y_spans[n]
        landed(two_z[n])
        t = gh[start:start + count, y, zi, zh]
        for s in range(7):
            t += rz2[s, start - 2:start - 2 + count]
        return coded(t)

    def pair_z(j):
        piece = code.at[pl.ds(j, 2), y, x, core, zi, zh]
        copies = [remote(piece, piece, dev(x, y, zp(s), core)) for s in range(1, 8)]
        launch(copies)
        return copies

    def pair_two(j):
        a, b = code.at[j, y, x, core], code.at[j + 1, y, x, core]
        copies = [remote(a, a, dev(x, yp(s), z, core)) for s in range(1, 4)]
        copies += [remote(b, b, dev(xp(s), y, z, core)) for s in range(1, 4)]
        launch(copies)
        return copies

    def pair_three(j):
        a, b = code.at[j, :, x, core], code.at[j + 1, y, :, core]
        one = [remote(a, a, dev(xp(s), y, z, core)) for s in range(1, 4)]
        two = [remote(b, b, dev(x, yp(s), z, core)) for s in range(1, 4)]
        launch(one + two)
        return one, two

    t = close(0)
    code[4:6, y, x, core, zi, zh] = t[0:2]
    code[6, y, x, core, zi, zh] = jnp.where(y == 3, scale, t[2].astype(F32)).astype(BF16)
    early = pair_z(5)
    piece = code.at[4, y, x, core, zi, zh]
    c1 = [remote(piece, piece, dev(x, yp(s), z, core)) for s in range(1, 4)]
    launch(c1)
    landed(two_y)
    code[0:2, y, x, core, zi, zh] = coded(gh[0:2, y, zi, zh] + ry2[0] + ry2[1] + ry2[2])
    other = pair_z(0)
    landed(c1)
    piece = code.at[4, :, x, core, zi, zh]
    c2 = [remote(piece, piece, dev(xp(s), y, z, core)) for s in range(1, 4)]
    launch(c2)
    code[2:4, y, x, core, zi, zh] = close(1)
    late = pair_z(2)
    landed(early)
    early = pair_two(5)
    landed(c2)
    piece = code.at[4, :, :, core, zi, zh]
    c3 = [remote(piece, piece, dev(x, y, zp(s), core)) for s in range(1, 8)]
    launch(c3)
    landed(other)
    other = pair_two(0)
    landed(early)
    early = pair_three(5)
    landed(late)
    late = pair_two(2)
    landed(other)
    other = pair_three(0)
    landed(late)
    late_a, late_b = pair_three(2)
    combine(2, mg, meta_g)
    for h in range(2):
        lanes = slice(h * 128, (h + 1) * 128)
        bias_out[:, lanes] = meta[3, 1 + h:2 + h]
        head_out[:, lanes] = meta[3, 3 + h:4 + h]

    def decode(first, js, t0, ts, x0, xs, half):
        def body(n, _):
            j, t, xx = first + n // (ts * xs), t0 + lax.rem(n // xs, ts), x0 + lax.rem(n, xs)
            inverse = 1.0 / code[6, 3, xx, half, 0, 0].astype(F32)[0:1]
            grown = inverse * ROOT
            for h in range(2):
                w = code[j, t, xx, half, :, h].astype(F32).reshape(32, 128)
                m = lax.rsqrt(lax.rsqrt(lax.rsqrt(lax.rsqrt(jnp.abs(w))))) * grown - inverse
                out_ref[j * 4 + t, pl.ds(xx * 64 + half * 32, 32), h * 128:(h + 1) * 128] = jnp.where(w < 0.0, -m, m)
            return 0

        lax.fori_loop(0, js * ts * xs, body, 0, unroll=4 if js * ts * xs % 4 == 0 else 1)

    handed = []

    def hand(j, js, t, ts, xx, xs):
        piece = code.at[pl.ds(j, js), pl.ds(t, ts), pl.ds(xx, xs), core]
        copy = remote(piece, piece, partner)
        launch([copy])
        handed.append((copy, j, js, t, ts, xx, xs))

    def show(j, js, t, ts, xx, xs, half):
        if j + js == 7:
            decode(5, 1, t, ts, xx, xs, half)
            decode(6, 1, 0, 3, xx, xs, half)
        else:
            decode(j, js, t, ts, xx, xs, half)

    def finish():
        copy, *place = handed.pop(0)
        copy.wait_recv()
        show(*place, 1 - core)

    hand(2, 1, 0, 4, x, 1)
    hand(3, 1, y, 1, 0, 4)
    landed(early[0] + early[1])
    handed, waiting = [], handed
    hand(5, 2, 0, 4, 0, 4)
    show(5, 2, 0, 4, 0, 4, core)
    landed(c3)
    hand(4, 1, 0, 4, 0, 4)
    show(4, 1, 0, 4, 0, 4, core)
    landed(other[0] + other[1])
    hand(0, 2, 0, 4, 0, 4)
    finish()
    handed += waiting
    show(2, 1, 0, 4, x, 1, core)
    show(3, 1, y, 1, 0, 4, core)
    for s in (1, 3, 2):
        late_a[s - 1].wait_recv()
        hand(2, 1, 0, 4, xp(4 - s), 1)
        late_b[s - 1].wait_recv()
        hand(3, 1, yp(4 - s), 1, 0, 4)
        if s == 1:
            show(0, 2, 0, 4, 0, 4, core)
            finish()
        show(2, 1, 0, 4, xp(4 - s), 1, core)
        show(3, 1, yp(4 - s), 1, 0, 4, core)
        if s == 3:
            finish()
    while handed:
        finish()
    for can_send, copies in sends:
        @pl.when(can_send)
        def _():
            for copy in copies:
                copy.wait_send()


PARTS = 9


def put(gw_ref, bias_ref, head_ref, out_hbm, bias_hbm, head_hbm, sems):
    size = 27 // PARTS
    copies = [
        pltpu.make_async_copy(gw_ref.at[pl.ds(n * size, size)], out_hbm.at[pl.ds(n * size, size)], sems.at[n])
        for n in range(PARTS)
    ]
    copies.append(pltpu.make_async_copy(bias_ref, bias_hbm, sems.at[PARTS]))
    copies.append(pltpu.make_async_copy(head_ref, head_hbm, sems.at[PARTS + 1]))
    for copy in copies:
        copy.start()
    for copy in copies:
        copy.wait()


def per_device(clips, weight, bias, head):
    vm = pltpu.VMEM
    field = lambda w: vm((4, 4, w, C), BF16)
    cells = vm((4, 8, C), F32)
    cat = vm((4, 6, 32, 768), BF16)
    plane = vm((256, C), F32)
    turned, left = vm((8, 2, 32, 128), BF16), vm((6, 4, 32, 128), BF16)
    wide, right = vm((9, 6, 32, 512), BF16), vm((4, 4, 128, C), BF16)
    coded = (7, 4, 4, 2, 4, 2, 8, 128)
    scratch = [
        vm((2, 128, C), BF16), vm((1, C), F32), vm((1, C), F32),
        vm((9, 768, C), BF16), vm((9, 768, C), BF16), vm((4, 2, 40, C), BF16), field(40), cat,
        field(32), cells, cells, cat, field(32), cells, cells, cat,
        vm((2, 2, 8, C), F32), vm((2, 2, 8, C), F32), vm((2, 4, 32, C), F32), plane, plane, plane,
        vm((2, 128, C), BF16), vm((2, 128, C), BF16),
        turned, turned, left, left, wide, wide, right, right, vm((864, C), F32),
        vm((7, 4, 4, 2, 8, 128), F32), vm(coded, BF16),
        vm((3, 5, 4, 2, 8, 128), F32), vm((7, 2, 4, 8, 128), F32), vm((3, 2, 8, 128), F32),
        vm((7, 5, 8, 128), F32),
        vm((4, 8, 128), F32), vm((8, 8, 128), F32), vm((4, 8, 128), F32), vm((8, 8, 128), F32),
        pltpu.SemaphoreType.DMA((4,)),
        pltpu.SemaphoreType.DMA((NREMOTE,)), pltpu.SemaphoreType.DMA((NREMOTE,)),
    ]
    inside = pl.BlockSpec(memory_space=pltpu.VMEM)
    outside = pl.BlockSpec(memory_space=pltpu.HBM)
    gw, grad_bias, grad_head = pl.pallas_call(
        kernel,
        out_shape=(pltpu.VMEM((27, C, C), F32), pltpu.VMEM((1, C), F32), pltpu.VMEM((1, C), F32)),
        in_specs=[outside] * 4,
        out_specs=(inside, inside, inside),
        scratch_shapes=scratch,
        compiler_params=pltpu.CompilerParams(
            collective_id=0, has_side_effects=True, vmem_limit_bytes=48 * 1024 * 1024
        ),
        name="section",
    )(clips.reshape(2, 128, C), weight.reshape(9, 768, C), bias.reshape(1, C), head.reshape(1, C))
    gw, grad_bias, grad_head = pl.pallas_call(
        put,
        out_shape=(
            jax.ShapeDtypeStruct((27, C, C), F32),
            jax.ShapeDtypeStruct((1, C), F32),
            jax.ShapeDtypeStruct((1, C), F32),
        ),
        in_specs=[inside, inside, inside],
        out_specs=(outside, outside, outside),
        scratch_shapes=[pltpu.SemaphoreType.DMA((PARTS + 2,))],
        compiler_params=pltpu.CompilerParams(vmem_limit_bytes=16 * 1024 * 1024),
        name="put",
    )(gw, grad_bias, grad_head)
    return gw.reshape(3, 3, 3, C, C), grad_bias.reshape(C), grad_head.reshape(C)


def solution(mesh):
    return jax.shard_map(
        per_device,
        mesh=mesh,
        in_specs=(P("dp", "tm", "rows", None, None), P(), P(), P()),
        out_specs=(P(), P(), P()),
        check_vma=False,
    )
```
